32 devices in a mesh: wide: 8 (over z, y), narrow: 4 (over x, core).
Axes of the slice: x: 2, y: 2, z: 4, core: 2. Of those that a mesh axis runs over, the one named last changes fastest.
Arguments:
- rhs: float32 [3, 32, 32, 128], P(None, 'wide', 'narrow'), may hold values from -12 to 12
- start: float32 [3, 32, 32, 128], P(None, 'wide', 'narrow'), may hold values from -2 to 2
- trans: float32 [3, 32, 32, 128], P(None, 'wide', 'narrow'), may hold values from 0.2 to 2
- accum: float32 [32, 32, 128], P('wide', 'narrow'), may hold values from 2 to 8
- coupling: float32 [3, 3, 32, 32, 128], P(None, None, 'wide', 'narrow'), may hold values from -0.3 to 0.3
- well_cells: int32 [8, 4, 64], P('wide', 'narrow'), may hold values from 0 to 4095
- well_index: float32 [8, 4, 64], P('wide', 'narrow'), may hold values from 1 to 20
- agg_map: int32 [32, 32, 128], P('wide', 'narrow'), may hold values from 0 to 31
- tile_factors: bfloat16 [48, 48, 128, 128], P('wide', 'narrow')
- coarse_inverse: float32 [1024, 1024], P(('wide', 'narrow')), as said below
Outputs:
- iterate: float32 [3, 32, 32, 128], P(None, 'wide', 'narrow')
- residual: float32 [3, 32, 32, 128], P(None, 'wide', 'narrow')
The draws below stay inside these ranges and needn't reach their ends.
Inputs may be any that keep to these rules, and one draw needn't show every extreme that they name: well_cells names, for each device's 64 connections, one of that device's own 4 * 8 * 128 cells, counted by pair, then column, then position in the tile; connections may share a cell. agg_map names one of the 32 aggregates of the device that owns the cell. coarse_inverse is symmetric.
All inputs are finite; a program needn't handle non-finite values.
Results may differ from the reference program's by a relative error of at most 0.00095.
Values sent between devices are 32-bit elements; how exact they have to be, the bound alone decides.
A program may use at most 64 MiB of HBM per device.

```python
import math
import jax
import jax.numpy as jnp
from jax import lax

PHASES = 3
PX = 4
CY = 8
AGG_LOC = 32
CONN = 64
SWEEPS = 3
INNER = 3
TILE = 128
NX2 = 32
NY = 32
TX_ALL = 48
TY_ALL = 48
NAGG = 1024
N_WIDE = 8
N_NARROW = 4


def draw_tile_factors(key, part):
    full_shape = (TX_ALL, TY_ALL, TILE, TILE)
    deviation = 0.02 * jax.random.normal(key, full_shape, jnp.float32)
    return (jnp.eye(TILE, dtype=jnp.float32) + deviation).astype(jnp.bfloat16)


def draw_coarse_inverse(key, part):
    subkeys = jax.random.split(jax.random.fold_in(key, 7), 4)
    owners = NAGG // AGG_LOC
    shuffle = jax.random.permutation(subkeys[0], owners)
    position = jnp.argsort(shuffle)
    partner = shuffle[position ^ 1]
    device_of = jnp.arange(NAGG) // AGG_LOC
    paired = partner[device_of][:, None] == device_of[None, :]
    background = jax.random.normal(subkeys[1], (NAGG, NAGG), jnp.float32)
    partner_part = jax.random.normal(subkeys[2], (NAGG, NAGG), jnp.float32)
    diag_scale = jax.random.uniform(subkeys[3], (NAGG,), jnp.float32, 0.0005, 0.0015)
    back_scale = 5e-06
    sym_back = (background + background.T) * (back_scale / math.sqrt(2.0))
    sym_partner = (partner_part + partner_part.T) * (0.0004 / math.sqrt(2.0))
    return jnp.diag(diag_scale) + sym_back + jnp.where(paired, sym_partner, 0.0)


def set_ends(values, rng, smallest, high):
    longest = values.shape.index(max(values.shape))
    spots = []
    for shift in (0, 1):
        where = [jax.random.randint(jax.random.fold_in(rng, axis), (), 0, length) for axis, length in enumerate(values.shape)]
        where[longest] = (where[longest] + shift) % values.shape[longest]
        spots.append(tuple(where))
    return values.at[spots[0]].set(smallest).at[spots[1]].set(high)


def level_of(rng, shape, shards, least, largest):
    factor_of, own = 1.0, jax.random.fold_in(rng, 6)
    for dim, parts in shards:
        draws = jnp.exp(jax.random.uniform(jax.random.fold_in(own, dim), (parts,), jnp.float32, least / len(shards), largest / len(shards)))
        factor_of = factor_of * jnp.repeat(draws, shape[dim] // parts).reshape([-1 if axis == dim else 1 for axis in range(len(shape))])
    return factor_of


def normal_values(own_key, extent, width, limit, pieces=(), kind=jnp.bfloat16):
    entries = width * jax.random.normal(own_key, extent, jnp.float32)
    if pieces:
        entries = entries * level_of(own_key, extent, pieces, -0.22, 0.18)
    return jnp.clip(entries, -limit, limit).astype(kind)


def setup_inputs(seed: int = 0) -> dict:
    key_of = jax.random.split(jax.random.key(seed), 11)
    rhs = normal_values(key_of[0], (PHASES, NX2, NY, TILE), 2.0, 12.0, ((1, 8), (2, 4)), jnp.float32)
    start = normal_values(key_of[1], (PHASES, NX2, NY, TILE), 0.3, 2.0, ((1, 8), (2, 4)), jnp.float32)
    trans = jnp.clip(jnp.exp(math.log(2.0) - 2.3025851 * jax.random.uniform(key_of[2], (3, NX2, NY, TILE), jnp.float32) ** level_of(key_of[2], (3, NX2, NY, TILE), ((1, 8), (2, 4)), -0.2, 0.2)), 0.2, 2.0)
    accum = jnp.clip(jnp.exp(math.log(8.0) - 1.3862944 * jax.random.uniform(key_of[3], (NX2, NY, TILE), jnp.float32) ** level_of(key_of[3], (NX2, NY, TILE), ((0, 8), (1, 4)), -0.2, 0.2)), 2.0, 8.0)
    coupling = jnp.clip(jax.random.uniform(key_of[4], (PHASES, PHASES, NX2, NY, TILE), jnp.float32, -0.3, 0.3) * level_of(key_of[4], (PHASES, PHASES, NX2, NY, TILE), ((2, 8), (3, 4)), -0.4, 0.0), -0.3, 0.3)
    well_cells = set_ends(jax.random.randint(key_of[5], (N_WIDE, N_NARROW, CONN), 0, PX * CY * TILE), jax.random.fold_in(key_of[5], 1), 0, (PX * CY * TILE) - 1).astype(jnp.int32)
    well_index = jnp.clip(jnp.exp(math.log(20.0) - 2.9957323 * jax.random.uniform(key_of[6], (N_WIDE, N_NARROW, CONN), jnp.float32) ** level_of(key_of[6], (N_WIDE, N_NARROW, CONN), ((0, 8), (1, 4)), -0.2, 0.2)), 1.0, 20.0)
    agg_map = set_ends(jax.random.randint(key_of[7], (NX2, NY, TILE), 0, AGG_LOC), jax.random.fold_in(key_of[7], 1), 0, AGG_LOC - 1).astype(jnp.int32)
    tile_factors = draw_tile_factors(jax.random.fold_in(key_of[10], 71), 0)
    coarse_inverse = draw_coarse_inverse(jax.random.fold_in(key_of[10], 71), 0)
    return {"rhs": rhs, "start": start, "trans": trans, "accum": accum, "coupling": coupling, "well_cells": well_cells, "well_index": well_index, "agg_map": agg_map, "tile_factors": tile_factors, "coarse_inverse": coarse_inverse}


best_precision = lax.Precision.HIGHEST


def neighbour(values, along, offset, periodic):
    along = along % values.ndim
    if periodic:
        return jnp.roll(values, -offset, axis=along)
    length = values.shape[along]
    padding = [(0, 0)] * values.ndim
    if offset > 0:
        padding[along] = (0, offset)
        return lax.slice_in_dim(jnp.pad(values, padding), offset, offset + length, axis=along)
    padding[along] = (-offset, 0)
    return lax.slice_in_dim(jnp.pad(values, padding), 0, length, axis=along)


def east_of(values, periodic):
    middle = values.shape[-1] // 2
    from_next = neighbour(values, -3, 1, periodic)[..., :middle]
    return jnp.concatenate([values[..., middle:], from_next], axis=-1)


def west_of(values, periodic):
    middle = values.shape[-1] // 2
    from_prev = neighbour(values, -3, -1, periodic)[..., middle:]
    return jnp.concatenate([from_prev, values[..., :middle]], axis=-1)


def prepare(trans, accum_w, periodic):
    middle = trans.shape[-1] // 2
    layer_no = lax.broadcasted_iota(jnp.int32, accum_w.shape, accum_w.ndim - 1) % middle
    trans_x = trans[0]
    trans_y = trans[1]
    trans_z = jnp.where(layer_no < middle - 1, trans[2], 0.0)
    face_sum = trans_x + west_of(trans_x, periodic) + trans_y + neighbour(trans_y, -2, -1, periodic)
    face_sum = face_sum + trans_z + neighbour(trans_z, -1, -1, False)
    return trans_x, trans_y, trans_z, accum_w + face_sum


def operate(values, trans_x, trans_y, trans_z, centre, coupling, periodic):
    mixing = jnp.sum(coupling * values[None], axis=1)
    inflow = trans_x * east_of(values, periodic) + west_of(trans_x, periodic) * west_of(values, periodic)
    inflow = inflow + trans_y * neighbour(values, -2, 1, periodic)
    inflow = inflow + neighbour(trans_y, -2, -1, periodic) * neighbour(values, -2, -1, periodic)
    inflow = inflow + trans_z * neighbour(values, -1, 1, False)
    inflow = inflow + neighbour(trans_z, -1, -1, False) * neighbour(values, -1, -1, False)
    return centre * values + mixing - inflow


def tile_apply(values, inverse_diag, factors):
    scaled = (inverse_diag * values).astype(jnp.bfloat16)
    return jnp.einsum("cpyj,pykj->cpyk", scaled.astype(jnp.float32), factors.astype(jnp.float32), precision=best_precision)


def local_solve(misfit, coeffs, inverse_diag, factors):
    trans_x, trans_y, trans_z, centre, coupling = coeffs
    update = tile_apply(misfit, inverse_diag, factors)
    for _ in range(INNER - 1):
        applied = operate(update, trans_x, trans_y, trans_z, centre, coupling, False)
        update = update + tile_apply(misfit - applied, inverse_diag, factors)
    return update


def wrap_pad(values):
    widths = ((1, 1), (2, 2), (0, 0))
    return jnp.pad(values, ((0, 0),) * (values.ndim - 3) + widths, mode="wrap")


def subdomains(misfit_pad, padded, tile_factors):
    def one_device(device_no):
        wide_pos = (device_no // N_NARROW).astype(jnp.int32)
        narrow_pos = (device_no % N_NARROW).astype(jnp.int32)
        zero = jnp.zeros((), jnp.int32)

        def window(values):
            cut_x = lax.dynamic_slice_in_dim(values, (wide_pos * PX).astype(jnp.int32), PX + 2, values.ndim - 3)
            return lax.dynamic_slice_in_dim(cut_x, (narrow_pos * CY).astype(jnp.int32), CY + 4, values.ndim - 2)

        coeffs = [window(member) for member in padded[:5]]
        starts = ((wide_pos * (PX + 2)).astype(jnp.int32), (narrow_pos * (CY + 4)).astype(jnp.int32), zero, zero)
        factors = lax.dynamic_slice(tile_factors, starts, (PX + 2, CY + 4, TILE, TILE))
        update = local_solve(window(misfit_pad), coeffs, window(padded[5]), factors)
        return update[:, 1:-1, 2:-2, :]

    blocks = lax.map(one_device, jnp.arange(N_WIDE * N_NARROW, dtype=jnp.int32))
    blocks = blocks.reshape(N_WIDE, N_NARROW, PHASES, PX, CY, TILE)
    return blocks.transpose(2, 0, 3, 1, 4, 5).reshape(PHASES, N_WIDE * PX, N_NARROW * CY, TILE)


def reference(rhs, start, trans, accum, coupling, well_cells, well_index, agg_map, tile_factors, coarse_inverse):
    flat_local = well_cells.astype(jnp.int32)
    pair_pos = jnp.arange(N_WIDE, dtype=jnp.int32)[:, None, None] * PX + flat_local // (CY * TILE)
    row_pos = jnp.arange(N_NARROW, dtype=jnp.int32)[None, :, None] * CY + (flat_local // TILE) % CY
    cell_pos = flat_local % TILE
    accum_w = accum.at[pair_pos, row_pos, cell_pos].add(well_index)
    trans_x, trans_y, trans_z, centre = prepare(trans, accum_w, True)
    coupling_diag = jnp.stack([coupling[member, member] for member in range(PHASES)])
    inverse_diag = 1.0 / (centre[None] + coupling_diag)
    padded = [wrap_pad(member) for member in (trans_x, trans_y, trans_z, centre, coupling, inverse_diag)]
    owner_no = (lax.broadcasted_iota(jnp.int32, accum.shape, 0) // PX) * N_NARROW
    owner_no = owner_no + lax.broadcasted_iota(jnp.int32, accum.shape, 1) // CY
    group_ids = (owner_no * AGG_LOC + agg_map.astype(jnp.int32)).reshape(-1)
    current = start
    for _ in range(SWEEPS):
        misfit = rhs - operate(current, trans_x, trans_y, trans_z, centre, coupling, True)
        correction = subdomains(wrap_pad(misfit), padded, tile_factors)
        coarse_rhs = jax.ops.segment_sum(misfit[0].reshape(-1), group_ids, num_segments=NAGG)
        coarse_sol = jnp.dot(coarse_inverse, coarse_rhs, precision=best_precision)
        correction = correction.at[0].add(coarse_sol[group_ids].reshape(accum.shape))
        current = current + correction
    final_misfit = rhs - operate(current, trans_x, trans_y, trans_z, centre, coupling, True)
    return current, final_misfit
```

```python
import functools

import jax
import jax.numpy as jnp
from jax import lax
from jax.experimental import pallas as pl
from jax.experimental.pallas import tpu as pltpu
from jax.sharding import PartitionSpec as P

SWEEPS = 3
HIGHEST = lax.Precision.HIGHEST
NT = (((1,), (1,)), ((), ()))
F32 = jnp.float32

DIRS = ((-1, 0), (1, 0), (0, -1), (0, 1), (-1, -1), (-1, 1), (1, -1), (1, 1))
UP_FIRST = (1, 6, 7, 2, 3, 0, 4, 5)
DOWN_FIRST = (0, 4, 5, 2, 3, 1, 6, 7)
ACW, TX, TY, TZ = range(4)


def slot(t, cy):
    if t < cy:
        return t + 2
    return t + 2 if t < cy + 2 else t - cy - 2


def halo_piece(d, px, cy, depth_x, depth_y):
    dx, dy = d
    if dx == 0:
        sp, dp, npair = 2, 2, px
    elif dx > 0:
        sp, dp, npair = 2 + px - depth_x, 2 - depth_x, depth_x
    else:
        sp, dp, npair = 2, 2 + px, depth_x
    if dy == 0:
        sr, dr, nrow = 0, 0, cy
    elif dy > 0:
        sr, dr, nrow = cy - depth_y, 2 * cy - depth_y, depth_y
    else:
        sr, dr, nrow = 0, cy, depth_y
    return (pl.ds(sp, npair), pl.ds(sr, nrow)), (pl.ds(dp, npair), pl.ds(dr, nrow))


def body(
    nw, nn,
    rhs, start, trans, accum, coupling, cells, widx, agg, tiles, cinv,
    out_it, out_res,
    COEF, CUR, FIX, W1, W2, H, DER, TF, WT, CI, AG, AGX, ACC, CELLS, WIDX, GB, YB,
    loc, hs, hr, cs, cr, gs, gr, is_, ir, near, far,
):
    phases = rhs.shape[0]
    px, cy, tile = accum.shape
    box = px + 2
    half = tile // 2
    aggs = CI.shape[0]
    me_w, me_n = lax.axis_index("wide"), lax.axis_index("narrow")

    def dev(dw, dn):
        return {"wide": lax.rem(me_w + dw + nw, nw), "narrow": lax.rem(me_n + dn + nn, nn)}

    own = pl.ds(2, px)
    top = pl.ds(0, cy)
    nch = COEF.shape[0]
    first_rhs = nch - phases
    copies = [
        (cells, CELLS),
        (widx, WIDX),
        (accum, ACC),
        (trans, COEF.at[pl.ds(1, 3), own, top]),
        (start, CUR.at[0, :, own, top]),
        (coupling, COEF.at[pl.ds(4, phases * phases), own, top]),
        (rhs, COEF.at[pl.ds(first_rhs, phases), own, top]),
        (agg, AG),
        (cinv, CI),
        (tiles, TF),
    ]
    local = [pltpu.make_async_copy(s, d, loc.at[k]) for k, (s, d) in enumerate(copies)]
    for c in local:
        c.start()

    peers = [(dw, dn) for dw in range(nw) for dn in range(nn) if dw or dn]

    def signal(sem, d):
        pl.semaphore_signal(sem, inc=1, device_id=dev(*d), device_id_type=pl.DeviceIdType.MESH)

    barrier = pltpu.get_barrier_semaphore()
    for p in range(px + 4):
        AGX[p] = jnp.zeros((2 * cy, tile), jnp.int32)
    for d in DIRS:
        signal(barrier, d)

    def remote(src, dst, ss, rs, d):
        return pltpu.make_async_remote_copy(
            src_ref=src, dst_ref=dst, send_sem=ss, recv_sem=rs,
            device_id=dev(*d), device_id_type=pl.DeviceIdType.MESH,
        )

    def halo(e):
        out = []
        for k, d in enumerate(DIRS):
            src, dst = halo_piece(d, px, cy, 2, 2 if d[0] else 3)
            out.append(remote(CUR.at[(e, slice(None)) + src], CUR.at[(e, slice(None)) + dst],
                              hs.at[e, k], hr.at[e, k], d))
        return out

    coef, bulk, late = [], ([], []), ([], [])

    def send_coef(channels, src, dst, d):
        k = len(coef)
        coef.append(remote(COEF.at[(channels,) + src], COEF.at[(channels,) + dst], cs.at[k], cr.at[k], d))
        return coef[-1]

    pieces = []
    for d in DIRS:
        depth_y = 1 if d[0] < 0 else 2
        src, dst = halo_piece(d, px, cy, 1, depth_y)
        main = [send_coef(pl.ds(1, nch - 1), src, dst, d)]
        rest = [send_coef(pl.ds(ACW, 1), src, dst, d)]
        if d[0] > 0:
            (_, sr), (_, dr) = src, dst
            rest.append(send_coef(pl.ds(1, 1), (pl.ds(px, 1), sr), (pl.ds(0, 1), dr), d))
        if d[1] > 0:
            (sp, _), (dp, _) = src, dst
            rest.append(send_coef(pl.ds(2, 1), (sp, pl.ds(cy - depth_y - 1, 1)), (dp, pl.ds(2 * cy - depth_y - 1, 1)), d))
        pieces.append((main, rest))
    for k in UP_FIRST:
        bulk[0].extend(pieces[k][0])
        late[0].extend(pieces[k][1])
    for k in DOWN_FIRST:
        bulk[1].extend(pieces[k][0])
        late[1].extend(pieces[k][1])

    aggregates = []
    for k, d in enumerate(DIRS):
        src, dst = halo_piece(d, px, cy, 2, 2 if d[0] else 3)
        aggregates.append(remote(AGX.at[src], AGX.at[dst], is_.at[k], ir.at[k], d))
    odd = lax.rem(me_w, 2)

    def start_all(first, second):
        @pl.when(odd == 1)
        def _():
            for c in first:
                c.start()

        @pl.when(odd == 0)
        def _():
            for c in second:
                c.start()

    local[4].wait()
    pl.semaphore_wait(barrier, len(DIRS))
    for d in DIRS:
        signal(near, d)
    begin = halo(0)
    start_all([begin[k] for k in UP_FIRST], [begin[k] for k in DOWN_FIRST])
    for c in (local[3], local[5], local[6]):
        c.wait()
    start_all(*bulk)
    conn = cells.shape[-1]
    for c in local[:3]:
        c.wait()
    cell_row = CELLS[...]
    rows_own = px * cy
    hit_r = lax.broadcasted_iota(jnp.int32, (rows_own, conn), 0) == cell_row // tile
    hit_l = lax.broadcasted_iota(jnp.int32, (tile, conn), 0) == cell_row % tile
    left = jnp.where(hit_r, jnp.broadcast_to(WIDX[...], (rows_own, conn)), 0.0)
    right = jnp.where(hit_l, 1.0, 0.0)
    wells = lax.dot_general(left, right, NT, precision=HIGHEST, preferred_element_type=F32)
    COEF[ACW, 2 : 2 + px, 0:cy, :] = ACC[...] + wells.reshape(px, cy, tile)
    start_all(*late)
    local[7].wait()
    AGX[2 : 2 + px, 0:cy] = (AG[...] + me_n * aggs).reshape(px, cy, tile)
    for c in aggregates:
        c.start()

    lane = lax.broadcasted_iota(jnp.int32, (2 * cy, tile), 1)
    low = lane < half
    roll = pltpu.roll

    zero16 = jnp.zeros((2 * cy, tile), F32)
    for c in range(phases):
        for w in (W1, W2):
            w[c, 0] = zero16
            w[c, box + 1] = zero16
        W2[c, 1] = zero16
        W2[c, box] = zero16
    local[9].wait()
    half_y = cy // 2
    for b in range(box):
        for t in range(cy + 4):
            if t < cy:
                kb, nb = t % half_y, t // half_y
            else:
                kb, nb = half_y + (t - cy) % 2, (t - cy) // 2
            WT[b, kb * tile : (kb + 1) * tile, nb * tile : (nb + 1) * tile] = TF[b, slot(t, cy)].T
    pl.semaphore_wait(near, len(DIRS))
    reach, k = 2, 0
    while reach < max(nw // 2, nn // 2):
        ws = (0,) if reach >= nw // 2 else (-reach, 0, reach)
        ns = (0,) if reach >= nn // 2 else (-reach, 0, reach)
        ring_of = [(a, c) for a in ws for c in ns if a or c]
        for d in ring_of:
            signal(far.at[k], d)
        pl.semaphore_wait(far.at[k], len(ring_of))
        reach, k = 2 * reach, k + 1
    local[8].wait()
    for c in coef:
        c.wait_recv()

    for b in range(box):
        tx = COEF[TX, b + 1]
        txw = jnp.where(low, roll(COEF[TX, b], half, 1), roll(tx, half, 1))
        ty = COEF[TY, b + 1]
        tys = roll(ty, 1, 0)
        tz = jnp.where(lane % half < half - 1, COEF[TZ, b + 1], 0.0)
        tzd = roll(tz, 1, 1)
        centre = COEF[ACW, b + 1] + (tx + txw + ty + tys + tz + tzd)
        DER[0, b] = txw
        DER[1, b] = tys
        DER[2, b] = tz
        DER[3, b] = tzd
        for c in range(phases):
            diag = centre + COEF[4 + c * phases + c, b + 1]
            DER[4 + c, b] = diag
            DER[4 + phases + c, b] = 1.0 / diag

    def operate(read, boxes):
        swapped = {}

        def swap(c, idx):
            if (c, idx) not in swapped:
                swapped[c, idx] = roll(read(c, idx), half, 1)
            return swapped[c, idx]

        for b in boxes:
            values = [read(c, b + 1) for c in range(phases)]
            result = []
            for c in range(phases):
                v = values[c]
                east = jnp.where(low, swap(c, b + 1), swap(c, b + 2))
                west = jnp.where(low, swap(c, b), swap(c, b + 1))
                total = DER[4 + c, b] * v
                for o in range(phases):
                    if o != c:
                        total = total + COEF[4 + c * phases + o, b + 1] * values[o]
                inflow = COEF[TX, b + 1] * east + DER[0, b] * west
                inflow = inflow + COEF[TY, b + 1] * roll(v, 2 * cy - 1, 0)
                inflow = inflow + DER[1, b] * roll(v, 1, 0)
                inflow = inflow + DER[2, b] * roll(v, tile - 1, 1)
                inflow = inflow + DER[3, b] * roll(v, 1, 1)
                result.append(total - inflow)
            yield b, result

    row = lax.broadcasted_iota(jnp.int32, (2 * cy, tile), 0)
    upper_half = ((row >= half_y) & (row < cy)) | (row >= 2 * cy - 2)
    own_blocks = [(row < cy) & (row % half_y == j) for j in range(half_y)]
    near_rows = (row == cy, row == 2 * cy - 1)
    ring_rows = ((row == cy) | (row == 2 * cy - 2), (row == cy + 1) | (row == 2 * cy - 1))

    def product(b, q, extra):
        n = cy if extra is None else 2 * cy
        blocks = own_blocks + list(extra or ())
        stack = jnp.concatenate([v[:n] for v in q], axis=0)
        masks = [jnp.concatenate([m[:n]] * phases, axis=0) for m in blocks]
        lhs = jnp.concatenate([jnp.where(m, stack, 0.0) for m in masks], axis=1).astype(jnp.bfloat16)
        out = jnp.dot(lhs, WT[b, : len(blocks) * tile, :], preferred_element_type=F32)
        return [jnp.where(upper_half[:n], out[c * n : (c + 1) * n, tile:], out[c * n : (c + 1) * n, :tile])
                for c in range(phases)]

    inner = range(1, box - 1)

    def scaled(b, h):
        return [DER[4 + phases + c, b] * h[c] for c in range(phases)]

    agg_iota = lax.broadcasted_iota(jnp.int32, (aggs, tile), 0)

    def current(e):
        return lambda c, idx: FIX[idx] if c == 0 else CUR[e, c, idx]

    def sweep(s, carry):
        read = current(s)
        acc = jnp.zeros((aggs, tile), F32)
        for b, applied in operate(read, inner):
            h = [COEF[first_rhs + c, b + 1] - applied[c] for c in range(phases)]
            for c in range(phases):
                H[c, b] = h[c]
            for y in range(cy):
                ids = AG[pl.ds((b - 1) * cy + y, 1), :]
                acc = acc + jnp.where(agg_iota == ids, h[0][y : y + 1], 0.0)
        sums = jnp.broadcast_to(jnp.sum(acc, axis=1, keepdims=True), (aggs, tile))
        for g in range(nw):
            y = jnp.sum(CI[:, g * tile : (g + 1) * tile] * sums, axis=0, keepdims=True)
            for k in range(3):
                YB[s, (g + 1 - k) % nw, k : k + 1] = y
        share = [remote(YB.at[s, lax.rem(me_w + d[0], nw)], GB.at[s, k], gs.at[s], gr.at[s], d)
                 for k, d in enumerate(peers)]
        for c in share:
            c.start()
        for b, applied in operate(read, (0, box - 1)):
            for c in range(phases):
                H[c, b] = COEF[first_rhs + c, b + 1] - applied[c]

        for b in range(box):
            out = product(b, scaled(b, [H[c, b] for c in range(phases)]), ring_rows if b in inner else near_rows)
            for c in range(phases):
                W1[c, b + 1] = out[c]

        for b, applied in operate(lambda c, idx: W1[c, idx], range(box)):
            q = scaled(b, [H[c, b] - applied[c] for c in range(phases)])
            out = product(b, q, near_rows if b in inner else None)
            n = 2 * cy if b in inner else cy
            for c in range(phases):
                W2[c, b + 1, :n] = W1[c, b + 1, :n] + out[c]

        for b, applied in operate(lambda c, idx: W2[c, idx], inner):
            out = product(b, scaled(b, [H[c, b] - applied[c] for c in range(phases)]), None)
            for c in range(phases):
                CUR[s + 1, c, b + 1, :cy] = read(c, b + 1)[:cy] + (W2[c, b + 1, :cy] + out[c])

        sent = halo(s + 1)
        start_all([sent[k] for k in UP_FIRST], [sent[k] for k in DOWN_FIRST])
        for c in halo(s):
            c.wait_send()
        pltpu.make_async_copy(GB.at[s], GB.at[s], gs.at[s]).wait()
        pltpu.make_async_copy(GB.at[s], GB.at[s], gr.at[s]).wait()
        total = YB[s, me_w]
        for k in range(len(peers)):
            total = total + GB[s, k]
        tables = [jnp.broadcast_to(total[k : k + 1], (2 * cy, tile)) for k in range(3)]
        for c in halo(s + 1):
            c.wait_recv()
        for p in range(px + 4):
            table = tables[0 if p < 2 else 1 if p < 2 + px else 2]
            lifted = jnp.take_along_axis(table, AGX[p], axis=1, mode="promise_in_bounds")
            FIX[p] = CUR[s + 1, 0, p] + lifted
        return carry

    for c in halo(0):
        c.wait_recv()
    for p in range(px + 4):
        FIX[p] = CUR[0, 0, p]
    for c in aggregates:
        c.wait_recv()
    lax.fori_loop(0, SWEEPS, sweep, 0)
    last = current(SWEEPS)
    for c in range(phases):
        for p in range(px):
            out_it[c, p] = last(c, p + 2)[:cy]
    for b, applied in operate(last, inner):
        for c in range(phases):
            out_res[c, b - 1] = COEF[first_rhs + c, b + 1, 0:cy] - applied[c][:cy]
    for c in halo(SWEEPS) + coef + aggregates:
        c.wait_send()


def solution(mesh):
    nw, nn = mesh.shape["wide"], mesh.shape["narrow"]

    def per_device(rhs, start, trans, accum, coupling, well_cells, well_index, agg_map, tile_factors, coarse_inverse):
        phases, px, cy, tile = rhs.shape
        box = px + 2
        aggs = coarse_inverse.shape[0]
        conn = well_cells.size
        nch = 4 + phases * phases + phases
        vmem = pl.BlockSpec(memory_space=pltpu.VMEM)
        hbm = pl.BlockSpec(memory_space=pl.ANY)
        shape = jax.ShapeDtypeStruct(rhs.shape, F32)
        ring = (2 * cy, tile)
        dma = pltpu.SemaphoreType.DMA
        call = pl.pallas_call(
            functools.partial(body, nw, nn),
            out_shape=(pltpu.VMEM(rhs.shape, F32), pltpu.VMEM(rhs.shape, F32)),
            in_specs=[hbm] * 10,
            out_specs=(vmem, vmem),
            scratch_shapes=[
                pltpu.VMEM((nch, px + 4) + ring, F32),
                pltpu.VMEM((SWEEPS + 1, phases, px + 4) + ring, F32),
                pltpu.VMEM((px + 4,) + ring, F32),
                pltpu.VMEM((phases, px + 4) + ring, F32),
                pltpu.VMEM((phases, px + 4) + ring, F32),
                pltpu.VMEM((phases, box) + ring, F32),
                pltpu.VMEM((4 + 2 * phases, box) + ring, F32),
                pltpu.VMEM(tile_factors.shape, tile_factors.dtype),
                pltpu.VMEM((box, (cy // 2 + 2) * tile, 2 * tile), tile_factors.dtype),
                pltpu.VMEM(coarse_inverse.shape, F32),
                pltpu.VMEM((px * cy, tile), jnp.int32),
                pltpu.VMEM((px + 4,) + ring, jnp.int32),
                pltpu.VMEM(accum.shape, F32),
                pltpu.VMEM((1, conn), jnp.int32),
                pltpu.VMEM((1, conn), F32),
                pltpu.VMEM((SWEEPS, nw * nn - 1, 3, tile), F32),
                pltpu.VMEM((SWEEPS, nw, 3, tile), F32),
                dma((10,)),
                dma((SWEEPS + 1, len(DIRS))),
                dma((SWEEPS + 1, len(DIRS))),
                dma((22,)),
                dma((22,)),
                dma((SWEEPS,)),
                dma((SWEEPS,)),
                dma((len(DIRS),)),
                dma((len(DIRS),)),
                pltpu.SemaphoreType.REGULAR,
                pltpu.SemaphoreType.REGULAR((max(nw, nn),)),
            ],
            compiler_params=pltpu.CompilerParams(collective_id=0, has_side_effects=True),
            name="schwarz",
        )
        held = call(
            rhs, start, trans, accum,
            coupling.reshape((phases * phases,) + accum.shape),
            well_cells.reshape(1, -1), well_index.reshape(1, -1),
            agg_map.reshape(px * cy, tile), tile_factors, coarse_inverse)
        return held

    return jax.shard_map(
        per_device,
        mesh=mesh,
        in_specs=(
            P(None, "wide", "narrow", None),
            P(None, "wide", "narrow", None),
            P(None, "wide", "narrow", None),
            P("wide", "narrow", None),
            P(None, None, "wide", "narrow", None),
            P("wide", "narrow", None),
            P("wide", "narrow", None),
            P("wide", "narrow", None),
            P("wide", "narrow", None, None),
            P(("wide", "narrow"), None),
        ),
        out_specs=(P(None, "wide", "narrow", None), P(None, "wide", "narrow", None)),
        check_vma=False,
    )
```

```python
import functools

import jax
import jax.numpy as jnp
from jax import lax
from jax.experimental import pallas as pl
from jax.experimental.pallas import tpu as pltpu
from jax.sharding import PartitionSpec as P

SWEEPS = 3
HIGHEST = lax.Precision.HIGHEST
NT = (((1,), (1,)), ((), ()))
F32 = jnp.float32

DIRS = ((-1, 0), (1, 0), (0, -1), (0, 1), (-1, -1), (-1, 1), (1, -1), (1, 1))
UP_FIRST = (1, 6, 7, 2, 3, 0, 4, 5)
DOWN_FIRST = (0, 4, 5, 2, 3, 1, 6, 7)
ACW, TX, TY, TZ = range(4)


def slot(t, cy):
    if t < cy:
        return t + 2
    return t + 2 if t < cy + 2 else t - cy - 2


def mirror(me, k, n):
    out, bit = 0, 1
    while bit < n:
        own = lax.rem(me // bit, 2)
        out = out + bit * (1 - own if (k // bit) % 2 else own)
        bit *= 2
    return out


def halo_piece(d, px, cy, depth_x, depth_y):
    dx, dy = d
    if dx == 0:
        sp, dp, npair = 2, 2, px
    elif dx > 0:
        sp, dp, npair = 2 + px - depth_x, 2 - depth_x, depth_x
    else:
        sp, dp, npair = 2, 2 + px, depth_x
    if dy == 0:
        sr, dr, nrow = 0, 0, cy
    elif dy > 0:
        sr, dr, nrow = cy - depth_y, 2 * cy - depth_y, depth_y
    else:
        sr, dr, nrow = 0, cy, depth_y
    return (pl.ds(sp, npair), pl.ds(sr, nrow)), (pl.ds(dp, npair), pl.ds(dr, nrow))


def body(
    nw, nn,
    rhs, start, trans, accum, coupling, cells, widx, agg, tiles, cinv,
    out_it, out_res,
    COEF, CUR, FIX, W1, W2, H, DER, TF, WT, CI, AG, AGX, ACC, CELLS, WIDX, GB, YB, XT, YT,
    loc, hs, hr, cs, cr, gs, gr, is_, ir, ts, tr, near, far,
):
    phases = rhs.shape[0]
    px, cy, tile = accum.shape
    box = px + 2
    half = tile // 2
    aggs = CI.shape[0]
    me_w, me_n = lax.axis_index("wide"), lax.axis_index("narrow")

    def dev(dw, dn):
        return {"wide": lax.rem(me_w + dw + nw, nw), "narrow": lax.rem(me_n + dn + nn, nn)}

    own = pl.ds(2, px)
    top = pl.ds(0, cy)
    nch = COEF.shape[0]
    first_rhs = nch - phases
    copies = [
        (cells, CELLS),
        (widx, WIDX),
        (accum, ACC),
        (trans, COEF.at[pl.ds(1, 3), own, top]),
        (start, CUR.at[0, :, own, top]),
        (coupling, COEF.at[pl.ds(4, phases * phases), own, top]),
        (rhs, COEF.at[pl.ds(first_rhs, phases), own, top]),
        (agg, AG),
        (cinv, CI),
        (tiles, TF),
    ]
    local = [pltpu.make_async_copy(s, d, loc.at[k]) for k, (s, d) in enumerate(copies)]
    for c in local:
        c.start()

    pairs = [(a, c) for a in reversed(range(nw)) for c in reversed(range(nn)) if a or c]
    mirror_w = [mirror(me_w, a, nw) for a in range(nw)]
    mirror_n = [mirror(me_n, c, nn) for c in range(nn)]

    def signal(sem, d):
        pl.semaphore_signal(sem, inc=1, device_id=dev(*d), device_id_type=pl.DeviceIdType.MESH)

    barrier = pltpu.get_barrier_semaphore()
    for p in range(px + 4):
        AGX[p] = jnp.zeros((2 * cy, tile), jnp.int32)
    for d in DIRS:
        signal(barrier, d)

    def remote(src, dst, ss, rs, d):
        return pltpu.make_async_remote_copy(
            src_ref=src, dst_ref=dst, send_sem=ss, recv_sem=rs,
            device_id=dev(*d), device_id_type=pl.DeviceIdType.MESH,
        )

    def halo(e):
        out = []
        for k, d in enumerate(DIRS):
            src, dst = halo_piece(d, px, cy, 2, 2 if d[0] else 3)
            out.append(remote(CUR.at[(e, slice(None)) + src], CUR.at[(e, slice(None)) + dst],
                              hs.at[e, k], hr.at[e, k], d))
        return out

    coef, bulk, late = [], ([], []), ([], [])

    def send_coef(channels, src, dst, d):
        k = len(coef)
        coef.append(remote(COEF.at[(channels,) + src], COEF.at[(channels,) + dst], cs.at[k], cr.at[k], d))
        return coef[-1]

    pieces = []
    for d in DIRS:
        corner = d[0] != 0 and d[1] != 0
        depth_y = 1 if d[0] else 2
        src, dst = halo_piece(d, px, cy, 1, depth_y)
        skip = TY if corner and d[0] > 0 else TX
        main = [send_coef(pl.ds(skip, nch - skip), src, dst, d)]
        rest = [send_coef(pl.ds(ACW, 1), src, dst, d)]
        if corner and d[0] > 0:
            src2, dst2 = halo_piece(d, px, cy, 2, 2)
            rest.append(send_coef(pl.ds(TX, 1), src2, dst2, d))
        elif d[0] > 0:
            rest.append(send_coef(pl.ds(TX, 1), (pl.ds(px, 1), src[1]), (pl.ds(0, 1), dst[1]), d))
        if d[1] > 0:
            rest.append(send_coef(pl.ds(TY, 1), (src[0], pl.ds(cy - depth_y - 1, 1)), (dst[0], pl.ds(2 * cy - depth_y - 1, 1)), d))
        pieces.append((main, rest))
    thin = [
        remote(COEF.at[TX, px + 1, top], XT, ts.at[0], tr.at[0], (1, 0)),
        remote(COEF.at[TY, own, pl.ds(cy - 1, 1)], YT, ts.at[1], tr.at[1], (0, 1)),
    ]
    for k in UP_FIRST:
        bulk[0].extend(pieces[k][0])
        late[0].extend(pieces[k][1])
    for k in DOWN_FIRST:
        bulk[1].extend(pieces[k][0])
        late[1].extend(pieces[k][1])

    aggregates = []
    for k, d in enumerate(DIRS):
        src, dst = halo_piece(d, px, cy, 2, 2 if d[0] else 3)
        aggregates.append(remote(AGX.at[src], AGX.at[dst], is_.at[k], ir.at[k], d))
    odd = lax.rem(me_w, 2)

    def start_all(first, second):
        @pl.when(odd == 1)
        def _():
            for c in first:
                c.start()

        @pl.when(odd == 0)
        def _():
            for c in second:
                c.start()

    local[4].wait()
    pl.semaphore_wait(barrier, len(DIRS))
    for d in DIRS:
        signal(near, d)
    begin = halo(0)
    start_all([begin[k] for k in UP_FIRST], [begin[k] for k in DOWN_FIRST])
    local[3].wait()
    for c in thin:
        c.start()
    for c in (local[5], local[6]):
        c.wait()
    start_all(*bulk)
    conn = cells.shape[-1]
    for c in local[:3]:
        c.wait()
    cell_row = CELLS[...]
    rows_own = px * cy
    hit_r = lax.broadcasted_iota(jnp.int32, (rows_own, conn), 0) == cell_row // tile
    hit_l = lax.broadcasted_iota(jnp.int32, (tile, conn), 0) == cell_row % tile
    left = jnp.where(hit_r, jnp.broadcast_to(WIDX[...], (rows_own, conn)), 0.0)
    right = jnp.where(hit_l, 1.0, 0.0)
    wells = lax.dot_general(left, right, NT, precision=HIGHEST, preferred_element_type=F32)
    COEF[ACW, 2 : 2 + px, 0:cy, :] = ACC[...] + wells.reshape(px, cy, tile)
    start_all(*late)
    local[7].wait()
    AGX[2 : 2 + px, 0:cy] = (AG[...] + me_n * aggs).reshape(px, cy, tile)
    for c in aggregates:
        c.start()

    lane = lax.broadcasted_iota(jnp.int32, (2 * cy, tile), 1)
    low = lane < half
    roll = pltpu.roll

    zero16 = jnp.zeros((2 * cy, tile), F32)
    for c in range(phases):
        for w in (W1, W2):
            w[c, 0] = zero16
            w[c, box + 1] = zero16
        W2[c, 1] = zero16
        W2[c, box] = zero16
    rounds, reach = [], 2
    while reach < max(nw // 2, nn // 2):
        ws = (0,) if reach >= nw // 2 else (-reach, 0, reach)
        ns = (0,) if reach >= nn // 2 else (-reach, 0, reach)
        rounds.append([(a, c) for a in ws for c in ns if a or c])
        reach *= 2

    def join(opening):
        for k, group in enumerate(rounds):
            if opening == (k == 0):
                for d in group:
                    signal(far.at[k], d)
            if not opening:
                pl.semaphore_wait(far.at[k], len(group))

    pl.semaphore_wait(near, len(DIRS))
    join(True)
    local[9].wait()
    half_y = cy // 2
    for b in range(box):
        for t in range(cy + 4):
            if t < cy:
                kb, nb = t % half_y, t // half_y
            else:
                kb, nb = half_y + (t != cy and t != cy + 3), (t - cy) // 2
            WT[b, kb * tile : (kb + 1) * tile, nb * tile : (nb + 1) * tile] = TF[b, slot(t, cy)].T
    join(False)
    agg_iota = lax.broadcasted_iota(jnp.int32, (aggs, tile), 0)

    def gather(acc, p, h):
        for y in range(cy):
            ids = AG[pl.ds(p * cy + y, 1), :]
            acc = acc + jnp.where(agg_iota == ids, h[y : y + 1], 0.0)
        return acc

    def solve_coarse(s, acc):
        sums = jnp.broadcast_to(jnp.sum(acc, axis=1, keepdims=True), (aggs, tile))
        for g in range(nw):
            y = jnp.sum(CI[:, g * tile : (g + 1) * tile] * sums, axis=0, keepdims=True)
            for k in range(3):
                YB[s, (g + 1 - k) % nw, k : k + 1] = y
        return [
            pltpu.make_async_remote_copy(
                src_ref=YB.at[s, mirror_w[a]], dst_ref=GB.at[s, k], send_sem=gs.at[s], recv_sem=gr.at[s],
                device_id={"wide": mirror_w[a], "narrow": mirror_n[c]}, device_id_type=pl.DeviceIdType.MESH)
            for k, (a, c) in enumerate(pairs)]

    local[8].wait()
    begin = halo(0)
    for c in begin + thin:
        c.wait_recv()
    acc = jnp.zeros((aggs, tile), F32)
    for p in range(px):
        idx = p + 2
        v, e, w = CUR[0, 0, idx], CUR[0, 0, idx + 1, :cy], CUR[0, 0, idx - 1, :cy]
        o = v[:cy]
        lo = low[:cy]
        tx, ty, tz = (COEF[k, idx, :cy] for k in (TX, TY, TZ))
        txw = jnp.where(lo, roll(XT[...] if p == 0 else COEF[TX, idx - 1, :cy], half, 1), roll(tx, half, 1))
        tys = jnp.where(lax.broadcasted_iota(jnp.int32, (cy, tile), 0) == 0, YT[p], roll(ty, 1, 0))
        tz = jnp.where(lane[:cy] % half < half - 1, tz, 0.0)
        tzd = roll(tz, 1, 1)
        turned = roll(o, half, 1)
        total = (COEF[ACW, idx, :cy] + (tx + txw + ty + tys + tz + tzd) + COEF[4, idx, :cy]) * o
        for k in range(1, phases):
            total = total + COEF[4 + k, idx, :cy] * CUR[0, k, idx, :cy]
        inflow = tx * jnp.where(lo, turned, roll(e, half, 1)) + txw * jnp.where(lo, roll(w, half, 1), turned)
        inflow = inflow + ty * roll(v, 2 * cy - 1, 0)[:cy] + tys * roll(v, 1, 0)[:cy]
        inflow = inflow + tz * roll(o, tile - 1, 1) + tzd * roll(o, 1, 1)
        acc = gather(acc, p, COEF[first_rhs, idx, :cy] - (total - inflow))
    for c in solve_coarse(0, acc):
        c.start()
    for c in coef:
        c.wait_recv()

    for b in range(box):
        tx = COEF[TX, b + 1]
        txw = jnp.where(low, roll(COEF[TX, b], half, 1), roll(tx, half, 1))
        ty = COEF[TY, b + 1]
        tys = roll(ty, 1, 0)
        tz = jnp.where(lane % half < half - 1, COEF[TZ, b + 1], 0.0)
        tzd = roll(tz, 1, 1)
        centre = COEF[ACW, b + 1] + (tx + txw + ty + tys + tz + tzd)
        DER[0, b] = txw
        DER[1, b] = tys
        DER[2, b] = tz
        DER[3, b] = tzd
        for c in range(phases):
            diag = centre + COEF[4 + c * phases + c, b + 1]
            DER[4 + c, b] = diag
            DER[4 + phases + c, b] = 1.0 / diag

    def operate(read, boxes):
        swapped = {}

        def swap(c, idx):
            if (c, idx) not in swapped:
                swapped[c, idx] = roll(read(c, idx), half, 1)
            return swapped[c, idx]

        for b in boxes:
            values = [read(c, b + 1) for c in range(phases)]
            result = []
            for c in range(phases):
                v = values[c]
                east = jnp.where(low, swap(c, b + 1), swap(c, b + 2))
                west = jnp.where(low, swap(c, b), swap(c, b + 1))
                total = DER[4 + c, b] * v
                for o in range(phases):
                    if o != c:
                        total = total + COEF[4 + c * phases + o, b + 1] * values[o]
                inflow = COEF[TX, b + 1] * east + DER[0, b] * west
                inflow = inflow + COEF[TY, b + 1] * roll(v, 2 * cy - 1, 0)
                inflow = inflow + DER[1, b] * roll(v, 1, 0)
                inflow = inflow + DER[2, b] * roll(v, tile - 1, 1)
                inflow = inflow + DER[3, b] * roll(v, 1, 1)
                result.append(total - inflow)
            yield b, result

    row = lax.broadcasted_iota(jnp.int32, (2 * cy, tile), 0)
    upper_half = ((row >= half_y) & (row < cy)) | (row >= 2 * cy - 2)
    own_blocks = [(row < cy) & (row % half_y == j) for j in range(half_y)]
    near_rows = ((row == cy) | (row == 2 * cy - 1),)
    ring_rows = near_rows + ((row == cy + 1) | (row == 2 * cy - 2),)

    def product(b, q, extra):
        n = cy if extra is None else 2 * cy
        blocks = own_blocks + list(extra or ())
        stack = jnp.concatenate([v[:n] for v in q], axis=0)
        masks = [jnp.concatenate([m[:n]] * phases, axis=0) for m in blocks]
        lhs = jnp.concatenate([jnp.where(m, stack, 0.0) for m in masks], axis=1).astype(jnp.bfloat16)
        out = jnp.dot(lhs, WT[b, : len(blocks) * tile, :], preferred_element_type=F32)
        return [jnp.where(upper_half[:n], out[c * n : (c + 1) * n, tile:], out[c * n : (c + 1) * n, :tile])
                for c in range(phases)]

    inner = range(1, box - 1)

    def scaled(b, h):
        return [DER[4 + phases + c, b] * h[c] for c in range(phases)]

    def current(e):
        return lambda c, idx: FIX[idx] if c == 0 else CUR[e, c, idx]

    def drain(e):
        for c in halo(e):
            c.wait_send()

    def share_done(s, sem):
        pltpu.make_async_copy(GB.at[s], GB.at[s], sem.at[s]).wait()

    def run(up):
        order = tuple(range(box)) if up else tuple(reversed(range(box)))
        close, distant = order[:-2], order[-2:]
        behind = [k for k, d in enumerate(DIRS) if d[0] == (-1 if up else 1)]
        ahead = [k for k in range(len(DIRS)) if k not in behind]
        side = [k for k, d in enumerate(DIRS) if not d[0]]
        faraway = (px + 2, px + 3) if up else (0, 1)

        def lift(e, tables, slots):
            for p in slots:
                table = tables[0 if p < 2 else 1 if p < 2 + px else 2]
                lifted = jnp.take_along_axis(table, AGX[p], axis=1, mode="promise_in_bounds")
                FIX[p] = CUR[e, 0, p] + lifted

        def receive(e):
            share_done(e - 1, gs)
            landed = halo(e)
            for k in ahead:
                landed[k].wait_recv()
            share_done(e - 1, gr)
            total = YB[e - 1, me_w]
            for k in range(len(pairs)):
                total = total + GB[e - 1, k]
            tables = [jnp.broadcast_to(total[k : k + 1], (2 * cy, tile)) for k in range(3)]
            lift(e, tables, [p for p in range(px + 4) if p not in faraway])

            def rest():
                for k in behind:
                    landed[k].wait_recv()
                lift(e, tables, faraway)

            return rest

        def begin_box(read, boxes, acc):
            for b, applied in operate(read, boxes):
                h = [COEF[first_rhs + c, b + 1] - applied[c] for c in range(phases)]
                for c in range(phases):
                    H[c, b] = h[c]
                out = product(b, scaled(b, h), ring_rows if b in inner else near_rows)
                for c in range(phases):
                    W1[c, b + 1] = out[c]
                if acc is not None and b in inner:
                    acc = gather(acc, b - 1, h[0])
            return acc

        def sweep(s, first):
            read = current(s)
            if first:
                begin_box(read, order, None)
            else:
                rest = receive(s)
                acc = begin_box(read, close, jnp.zeros((aggs, tile), F32))
                rest()
                acc = begin_box(read, distant, acc)
                for c in solve_coarse(s, acc):
                    c.start()
            for b, applied in operate(lambda c, idx: W1[c, idx], order):
                q = scaled(b, [H[c, b] - applied[c] for c in range(phases)])
                out = product(b, q, near_rows if b in inner else None)
                n = 2 * cy if b in inner else cy
                for c in range(phases):
                    W2[c, b + 1, :n] = W1[c, b + 1, :n] + out[c]
            done = []
            for b, applied in operate(lambda c, idx: W2[c, idx], order[1:-1]):
                done.append((b, product(b, scaled(b, [H[c, b] - applied[c] for c in range(phases)]), None)))
            sent = halo(s + 1)
            for part, ks in ((done[:2], behind), (done[2:], [k for k in ahead if k not in side] + side)):
                for b, out in part:
                    for c in range(phases):
                        CUR[s + 1, c, b + 1, :cy] = read(c, b + 1)[:cy] + (W2[c, b + 1, :cy] + out[c])
                for k in ks:
                    sent[k].start()
            drain(s)
            if first:
                for c in coef + thin + aggregates:
                    c.wait_send()
                for c in aggregates:
                    c.wait_recv()

        def later(s, carry):
            sweep(s, False)
            return carry

        sweep(0, True)
        lax.fori_loop(1, SWEEPS, later, 0)
        rest = receive(SWEEPS)
        last = current(SWEEPS)
        for c in range(phases):
            for p in range(px):
                out_it[c, p] = last(c, p + 2)[:cy]

        def finish(boxes):
            for b, applied in operate(last, boxes):
                for c in range(phases):
                    out_res[c, b - 1] = COEF[first_rhs + c, b + 1, 0:cy] - applied[c][:cy]

        finish(close[1:])
        rest()
        finish(distant[:1])
        drain(SWEEPS)

    for p in range(px + 4):
        FIX[p] = CUR[0, 0, p]

    @pl.when(odd == 1)
    def _():
        run(True)

    @pl.when(odd == 0)
    def _():
        run(False)


def hand_over(iterate, residual, out_it, out_res, sem):
    moves = [
        pltpu.make_async_copy(iterate, out_it, sem.at[0]),
        pltpu.make_async_copy(residual, out_res, sem.at[1]),
    ]
    for c in moves:
        c.start()
    for c in moves:
        c.wait()


def solution(mesh):
    nw, nn = mesh.shape["wide"], mesh.shape["narrow"]

    def per_device(rhs, start, trans, accum, coupling, well_cells, well_index, agg_map, tile_factors, coarse_inverse):
        phases, px, cy, tile = rhs.shape
        box = px + 2
        aggs = coarse_inverse.shape[0]
        conn = well_cells.size
        nch = 4 + phases * phases + phases
        vmem = pl.BlockSpec(memory_space=pltpu.VMEM)
        hbm = pl.BlockSpec(memory_space=pl.ANY)
        shape = jax.ShapeDtypeStruct(rhs.shape, F32)
        ring = (2 * cy, tile)
        dma = pltpu.SemaphoreType.DMA
        call = pl.pallas_call(
            functools.partial(body, nw, nn),
            out_shape=(pltpu.VMEM(rhs.shape, F32), pltpu.VMEM(rhs.shape, F32)),
            in_specs=[hbm] * 10,
            out_specs=(vmem, vmem),
            scratch_shapes=[
                pltpu.VMEM((nch, px + 4) + ring, F32),
                pltpu.VMEM((SWEEPS + 1, phases, px + 4) + ring, F32),
                pltpu.VMEM((px + 4,) + ring, F32),
                pltpu.VMEM((phases, px + 4) + ring, F32),
                pltpu.VMEM((phases, px + 4) + ring, F32),
                pltpu.VMEM((phases, box) + ring, F32),
                pltpu.VMEM((4 + 2 * phases, box) + ring, F32),
                pltpu.VMEM(tile_factors.shape, tile_factors.dtype),
                pltpu.VMEM((box, (cy // 2 + 2) * tile, 2 * tile), tile_factors.dtype),
                pltpu.VMEM(coarse_inverse.shape, F32),
                pltpu.VMEM((px * cy, tile), jnp.int32),
                pltpu.VMEM((px + 4,) + ring, jnp.int32),
                pltpu.VMEM(accum.shape, F32),
                pltpu.VMEM((1, conn), jnp.int32),
                pltpu.VMEM((1, conn), F32),
                pltpu.VMEM((SWEEPS, nw * nn - 1, 3, tile), F32),
                pltpu.VMEM((SWEEPS, nw, 3, tile), F32),
                pltpu.VMEM((cy, tile), F32),
                pltpu.VMEM((px, 1, tile), F32),
                dma((10,)),
                dma((SWEEPS + 1, len(DIRS))),
                dma((SWEEPS + 1, len(DIRS))),
                dma((22,)),
                dma((22,)),
                dma((SWEEPS,)),
                dma((SWEEPS,)),
                dma((len(DIRS),)),
                dma((len(DIRS),)),
                dma((2,)),
                dma((2,)),
                pltpu.SemaphoreType.REGULAR,
                pltpu.SemaphoreType.REGULAR((max(nw, nn),)),
            ],
            compiler_params=pltpu.CompilerParams(collective_id=0, has_side_effects=True),
            name="schwarz",
        )
        held = call(
            rhs, start, trans, accum,
            coupling.reshape((phases * phases,) + accum.shape),
            well_cells.reshape(1, -1), well_index.reshape(1, -1),
            agg_map.reshape(px * cy, tile), tile_factors, coarse_inverse)
        held = [pltpu.with_memory_space_constraint(x, pltpu.VMEM) for x in held]
        return pl.pallas_call(
            hand_over, out_shape=(shape, shape), in_specs=[vmem, vmem], out_specs=(hbm, hbm),
            scratch_shapes=[dma((2,))], name="hand_over",
        )(*held)

    return jax.shard_map(
        per_device,
        mesh=mesh,
        in_specs=(
            P(None, "wide", "narrow", None),
            P(None, "wide", "narrow", None),
            P(None, "wide", "narrow", None),
            P("wide", "narrow", None),
            P(None, None, "wide", "narrow", None),
            P("wide", "narrow", None),
            P("wide", "narrow", None),
            P("wide", "narrow", None),
            P("wide", "narrow", None, None),
            P(("wide", "narrow"), None),
        ),
        out_specs=(P(None, "wide", "narrow", None), P(None, "wide", "narrow", None)),
        check_vma=False,
    )
```

```python
import functools

import jax
import jax.numpy as jnp
from jax import lax
from jax.experimental import pallas as pl
from jax.experimental.pallas import tpu as pltpu
from jax.sharding import PartitionSpec as P

SWEEPS = 3
HIGHEST = lax.Precision.HIGHEST
NT = (((1,), (1,)), ((), ()))
F32 = jnp.float32

DIRS = ((-1, 0), (1, 0), (0, -1), (0, 1), (-1, -1), (-1, 1), (1, -1), (1, 1))
FACES, CORNERS = DIRS[:4], DIRS[4:]
UP_FIRST = (1, 6, 7, 2, 3, 0, 4, 5)
DOWN_FIRST = (0, 4, 5, 2, 3, 1, 6, 7)
ACW, TX, TY, TZ = range(4)


def slot(t, cy):
    if t < cy:
        return t + 2
    return t + 2 if t < cy + 2 else t - cy - 2


def mirror(me, k, n):
    out, bit = 0, 1
    while bit < n:
        own = lax.rem(me // bit, 2)
        out = out + bit * (1 - own if (k // bit) % 2 else own)
        bit *= 2
    return out


def halo_piece(d, px, cy, depth_x, depth_y):
    dx, dy = d
    if dx == 0:
        sp, dp, npair = 2, 2, px
    elif dx > 0:
        sp, dp, npair = 2 + px - depth_x, 2 - depth_x, depth_x
    else:
        sp, dp, npair = 2, 2 + px, depth_x
    if dy == 0:
        sr, dr, nrow = 0, 0, cy
    elif dy > 0:
        sr, dr, nrow = cy - depth_y, 2 * cy - depth_y, depth_y
    else:
        sr, dr, nrow = 0, cy, depth_y
    return (pl.ds(sp, npair), pl.ds(sr, nrow)), (pl.ds(dp, npair), pl.ds(dr, nrow))


def body(
    nw, nn,
    rhs, start, trans, accum, coupling, cells, widx, agg, tiles, cinv,
    out_it, out_res,
    COEF, CUR, FIX, W1, W2, H, DER, TF, WT, CI, AG, AGX, ACC, CELLS, WIDX, GB, YB, XT, YT, SECOND, PACK, LAND,
    loc, hs, hr, cs, cr, gs, gr, is_, ir, ts, tr, near, far,
):
    phases = rhs.shape[0]
    px, cy, tile = accum.shape
    box = px + 2
    half = tile // 2
    aggs = CI.shape[0]
    me_w, me_n = lax.axis_index("wide"), lax.axis_index("narrow")

    def dev(dw, dn):
        return {"wide": lax.rem(me_w + dw + nw, nw), "narrow": lax.rem(me_n + dn + nn, nn)}

    own = pl.ds(2, px)
    top = pl.ds(0, cy)
    nch = COEF.shape[0]
    first_rhs = nch - phases
    copies = [
        (cells, CELLS),
        (widx, WIDX),
        (accum, ACC),
        (trans, COEF.at[pl.ds(1, 3), own, top]),
        (start, CUR.at[0, :, own, top]),
        (coupling, COEF.at[pl.ds(4, phases * phases), own, top]),
        (rhs, COEF.at[pl.ds(first_rhs, phases), own, top]),
        (agg, AG),
        (cinv, CI),
        (tiles, TF),
    ]
    local = [pltpu.make_async_copy(s, d, loc.at[k]) for k, (s, d) in enumerate(copies)]
    for c in local:
        c.start()

    pairs = [(a, c) for a in reversed(range(nw)) for c in reversed(range(nn)) if a or c]
    mirror_w = [mirror(me_w, a, nw) for a in range(nw)]
    mirror_n = [mirror(me_n, c, nn) for c in range(nn)]

    def signal(sem, d):
        pl.semaphore_signal(sem, inc=1, device_id=dev(*d), device_id_type=pl.DeviceIdType.MESH)

    barrier = pltpu.get_barrier_semaphore()
    for p in range(px + 4):
        AGX[p] = jnp.zeros((2 * cy, tile), jnp.int32)
    for d in DIRS:
        signal(barrier, d)

    def remote(src, dst, ss, rs, d):
        return pltpu.make_async_remote_copy(
            src_ref=src, dst_ref=dst, send_sem=ss, recv_sem=rs,
            device_id=dev(*d), device_id_type=pl.DeviceIdType.MESH,
        )

    def copy(src, dst, e, k, d):
        return remote(src, dst, hs.at[e, k], hr.at[e, k], d)

    def rings(e, depth_y):
        out = []
        for k, d in enumerate(FACES):
            src, dst = halo_piece(d, px, cy, 1, depth_y)
            out.append(copy(CUR.at[(e, slice(None)) + src], CUR.at[(e, slice(None)) + dst], e, k, d))
        return out

    def extras(e):
        n = len(FACES)
        out = [copy(SECOND.at[e, k], CUR.at[e, pl.ds(0, 2), 0 if d[0] > 0 else px + 3, top], e, n + k, d)
               for k, d in enumerate(FACES[:2])]
        return out + [copy(PACK.at[e, k], LAND.at[e, k], e, n + 2 + k, d) for k, d in enumerate(CORNERS)]

    def halo(e):
        return rings(e, 3) + extras(e)

    def pack(e):
        lower = lax.broadcasted_iota(jnp.int32, (cy, tile), 1) < half
        for k, d in enumerate(FACES[:2]):
            p = px if d[0] > 0 else 3
            one, two = CUR[e, 1, p, :cy], pltpu.roll(CUR[e, 2, p, :cy], half, 1)
            SECOND[e, k, 0] = CUR[e, 0, p, :cy]
            SECOND[e, k, 1] = jnp.where(lower, two, one) if d[0] > 0 else jnp.where(lower, one, two)
        for k, d in enumerate(CORNERS):
            p = px + 1 if d[0] > 0 else 2
            y0, y1 = (cy - 1, cy - 2) if d[1] > 0 else (0, 1)
            for c in range(phases):
                PACK[e, k, pl.ds(2 * c, 1)] = CUR[e, c, p, pl.ds(y0, 1)]
                PACK[e, k, pl.ds(2 * c + 1, 1)] = CUR[e, c, p, pl.ds(y1, 1)]
            for c in range(2):
                PACK[e, k, pl.ds(2 * phases + c, 1)] = SECOND[e, 1 if d[0] > 0 else 0, c, pl.ds(y0, 1)]

    def unpack(e, corners):
        for k in corners:
            d = CORNERS[k]
            p, q = (1, 0) if d[0] > 0 else (px + 2, px + 3)
            y0, y1 = (2 * cy - 1, 2 * cy - 2) if d[1] > 0 else (cy, cy + 1)
            for c in range(phases):
                CUR[e, c, p, pl.ds(y0, 1)] = LAND[e, k, pl.ds(2 * c, 1)]
                CUR[e, c, p, pl.ds(y1, 1)] = LAND[e, k, pl.ds(2 * c + 1, 1)]
            for c in range(2):
                CUR[e, c, q, pl.ds(y0, 1)] = LAND[e, k, pl.ds(2 * phases + c, 1)]

    coef, bulk, late = [], ([], []), ([], [])

    def send_coef(channels, src, dst, d):
        k = len(coef)
        coef.append(remote(COEF.at[(channels,) + src], COEF.at[(channels,) + dst], cs.at[k], cr.at[k], d))
        return coef[-1]

    pieces = []
    for d in DIRS:
        corner = d[0] != 0 and d[1] != 0
        depth_y = 1 if d[0] else 2
        src, dst = halo_piece(d, px, cy, 1, depth_y)
        skip = TY if corner and d[0] > 0 else TX
        main = [send_coef(pl.ds(skip, nch - skip), src, dst, d)]
        rest = [send_coef(pl.ds(ACW, 1), src, dst, d)]
        if corner and d[0] > 0:
            src2, dst2 = halo_piece(d, px, cy, 2, 2)
            rest.append(send_coef(pl.ds(TX, 1), src2, dst2, d))
        elif d[0] > 0:
            rest.append(send_coef(pl.ds(TX, 1), (pl.ds(px, 1), src[1]), (pl.ds(0, 1), dst[1]), d))
        if d[1] > 0:
            rest.append(send_coef(pl.ds(TY, 1), (src[0], pl.ds(cy - depth_y - 1, 1)), (dst[0], pl.ds(2 * cy - depth_y - 1, 1)), d))
        pieces.append((main, rest))
    thin = [
        remote(COEF.at[TX, px + 1, top], XT, ts.at[0], tr.at[0], (1, 0)),
        remote(COEF.at[TY, own, pl.ds(cy - 1, 1)], YT, ts.at[1], tr.at[1], (0, 1)),
    ]
    for k in UP_FIRST:
        bulk[0].extend(pieces[k][0])
        late[0].extend(pieces[k][1])
    for k in DOWN_FIRST:
        bulk[1].extend(pieces[k][0])
        late[1].extend(pieces[k][1])

    aggregates = []
    for k, d in enumerate(DIRS):
        src, dst = halo_piece(d, px, cy, 2, 2 if d[0] else 3)
        aggregates.append(remote(AGX.at[src], AGX.at[dst], is_.at[k], ir.at[k], d))
    odd = lax.rem(me_w, 2)

    def start_all(first, second):
        @pl.when(odd == 1)
        def _():
            for c in first:
                c.start()

        @pl.when(odd == 0)
        def _():
            for c in second:
                c.start()

    local[4].wait()
    pack(0)
    pl.semaphore_wait(barrier, len(DIRS))
    for d in DIRS:
        signal(near, d)
    begin = halo(0)
    for c in begin:
        c.start()
    local[3].wait()
    for c in thin:
        c.start()
    for c in (local[5], local[6]):
        c.wait()
    start_all(*bulk)
    conn = cells.shape[-1]
    for c in local[:3]:
        c.wait()
    cell_row = CELLS[...]
    rows_own = px * cy
    hit_r = lax.broadcasted_iota(jnp.int32, (rows_own, conn), 0) == cell_row // tile
    hit_l = lax.broadcasted_iota(jnp.int32, (tile, conn), 0) == cell_row % tile
    left = jnp.where(hit_r, jnp.broadcast_to(WIDX[...], (rows_own, conn)), 0.0)
    right = jnp.where(hit_l, 1.0, 0.0)
    wells = lax.dot_general(left, right, NT, precision=HIGHEST, preferred_element_type=F32)
    COEF[ACW, 2 : 2 + px, 0:cy, :] = ACC[...] + wells.reshape(px, cy, tile)
    start_all(*late)
    local[7].wait()
    AGX[2 : 2 + px, 0:cy] = (AG[...] + me_n * aggs).reshape(px, cy, tile)
    for c in aggregates:
        c.start()

    lane = lax.broadcasted_iota(jnp.int32, (2 * cy, tile), 1)
    low = lane < half
    roll = pltpu.roll

    zero16 = jnp.zeros((2 * cy, tile), F32)
    for c in range(phases):
        for w in (W1, W2):
            w[c, 0] = zero16
            w[c, box + 1] = zero16
        W2[c, 1] = zero16
        W2[c, box] = zero16
    rounds, reach = [], 2
    while reach < max(nw // 2, nn // 2):
        ws = (0,) if reach >= nw // 2 else (-reach, 0, reach)
        ns = (0,) if reach >= nn // 2 else (-reach, 0, reach)
        rounds.append([(a, c) for a in ws for c in ns if a or c])
        reach *= 2

    def join(opening):
        for k, group in enumerate(rounds):
            if opening == (k == 0):
                for d in group:
                    signal(far.at[k], d)
            if not opening:
                pl.semaphore_wait(far.at[k], len(group))

    pl.semaphore_wait(near, len(DIRS))
    join(True)
    local[9].wait()
    half_y = cy // 2
    for b in range(box):
        for t in range(cy + 4):
            if t < cy:
                kb, nb = t % half_y, t // half_y
            else:
                kb, nb = half_y + (t != cy and t != cy + 3), (t - cy) // 2
            WT[b, kb * tile : (kb + 1) * tile, nb * tile : (nb + 1) * tile] = TF[b, slot(t, cy)].T
    join(False)
    agg_iota = lax.broadcasted_iota(jnp.int32, (aggs, tile), 0)

    def gather(acc, p, h):
        for y in range(cy):
            ids = AG[pl.ds(p * cy + y, 1), :]
            acc = acc + jnp.where(agg_iota == ids, h[y : y + 1], 0.0)
        return acc

    def solve_coarse(s, acc):
        sums = jnp.broadcast_to(jnp.sum(acc, axis=1, keepdims=True), (aggs, tile))
        for g in range(nw):
            y = jnp.sum(CI[:, g * tile : (g + 1) * tile] * sums, axis=0, keepdims=True)
            for k in range(3):
                YB[s, (g + 1 - k) % nw, k : k + 1] = y
        return [
            pltpu.make_async_remote_copy(
                src_ref=YB.at[s, mirror_w[a]], dst_ref=GB.at[s, k], send_sem=gs.at[s], recv_sem=gr.at[s],
                device_id={"wide": mirror_w[a], "narrow": mirror_n[c]}, device_id_type=pl.DeviceIdType.MESH)
            for k, (a, c) in enumerate(pairs)]

    local[8].wait()
    begin = halo(0)
    for c in begin + thin:
        c.wait_recv()
    unpack(0, range(len(CORNERS)))
    acc = jnp.zeros((aggs, tile), F32)
    for p in range(px):
        idx = p + 2
        v, e, w = CUR[0, 0, idx], CUR[0, 0, idx + 1, :cy], CUR[0, 0, idx - 1, :cy]
        o = v[:cy]
        lo = low[:cy]
        tx, ty, tz = (COEF[k, idx, :cy] for k in (TX, TY, TZ))
        txw = jnp.where(lo, roll(XT[...] if p == 0 else COEF[TX, idx - 1, :cy], half, 1), roll(tx, half, 1))
        tys = jnp.where(lax.broadcasted_iota(jnp.int32, (cy, tile), 0) == 0, YT[p], roll(ty, 1, 0))
        tz = jnp.where(lane[:cy] % half < half - 1, tz, 0.0)
        tzd = roll(tz, 1, 1)
        turned = roll(o, half, 1)
        total = (COEF[ACW, idx, :cy] + (tx + txw + ty + tys + tz + tzd) + COEF[4, idx, :cy]) * o
        for k in range(1, phases):
            total = total + COEF[4 + k, idx, :cy] * CUR[0, k, idx, :cy]
        inflow = tx * jnp.where(lo, turned, roll(e, half, 1)) + txw * jnp.where(lo, roll(w, half, 1), turned)
        inflow = inflow + ty * roll(v, 2 * cy - 1, 0)[:cy] + tys * roll(v, 1, 0)[:cy]
        inflow = inflow + tz * roll(o, tile - 1, 1) + tzd * roll(o, 1, 1)
        acc = gather(acc, p, COEF[first_rhs, idx, :cy] - (total - inflow))
    for c in solve_coarse(0, acc):
        c.start()
    def derive(boxes):
        for b in boxes:
            tx = COEF[TX, b + 1]
            txw = jnp.where(low, roll(COEF[TX, b], half, 1), roll(tx, half, 1))
            ty = COEF[TY, b + 1]
            tys = roll(ty, 1, 0)
            tz = jnp.where(lane % half < half - 1, COEF[TZ, b + 1], 0.0)
            tzd = roll(tz, 1, 1)
            centre = COEF[ACW, b + 1] + (tx + txw + ty + tys + tz + tzd)
            DER[0, b] = txw
            DER[1, b] = tys
            DER[2, b] = tz
            DER[3, b] = tzd
            for c in range(phases):
                diag = centre + COEF[4 + c * phases + c, b + 1]
                DER[4 + c, b] = diag
                DER[4 + phases + c, b] = 1.0 / diag

    def operate(read, boxes, packed=False):
        swapped = {}

        def swap(c, idx):
            if packed and c == 2 and idx in (0, px + 3):
                return read(1, idx)
            if (c, idx) not in swapped:
                swapped[c, idx] = roll(read(c, idx), half, 1)
            return swapped[c, idx]

        for b in boxes:
            values = [read(c, b + 1) for c in range(phases)]
            result = []
            for c in range(phases):
                v = values[c]
                east = jnp.where(low, swap(c, b + 1), swap(c, b + 2))
                west = jnp.where(low, swap(c, b), swap(c, b + 1))
                total = DER[4 + c, b] * v
                for o in range(phases):
                    if o != c:
                        total = total + COEF[4 + c * phases + o, b + 1] * values[o]
                inflow = COEF[TX, b + 1] * east + DER[0, b] * west
                inflow = inflow + COEF[TY, b + 1] * roll(v, 2 * cy - 1, 0)
                inflow = inflow + DER[1, b] * roll(v, 1, 0)
                inflow = inflow + DER[2, b] * roll(v, tile - 1, 1)
                inflow = inflow + DER[3, b] * roll(v, 1, 1)
                result.append(total - inflow)
            yield b, result

    row = lax.broadcasted_iota(jnp.int32, (2 * cy, tile), 0)
    upper_half = ((row >= half_y) & (row < cy)) | (row >= 2 * cy - 2)
    own_blocks = [(row < cy) & (row % half_y == j) for j in range(half_y)]
    near_rows = ((row == cy) | (row == 2 * cy - 1),)
    ring_rows = near_rows + ((row == cy + 1) | (row == 2 * cy - 2),)

    def product(b, q, extra):
        n = cy if extra is None else 2 * cy
        blocks = own_blocks + list(extra or ())
        stack = jnp.concatenate([v[:n] for v in q], axis=0)
        masks = [jnp.concatenate([m[:n]] * phases, axis=0) for m in blocks]
        lhs = jnp.concatenate([jnp.where(m, stack, 0.0) for m in masks], axis=1).astype(jnp.bfloat16)
        out = jnp.dot(lhs, WT[b, : len(blocks) * tile, :], preferred_element_type=F32)
        return [jnp.where(upper_half[:n], out[c * n : (c + 1) * n, tile:], out[c * n : (c + 1) * n, :tile])
                for c in range(phases)]

    inner = range(1, box - 1)

    def scaled(b, h):
        return [DER[4 + phases + c, b] * h[c] for c in range(phases)]

    def current(e):
        return lambda c, idx: FIX[idx] if c == 0 else CUR[e, c, idx]

    def drain(e):
        for c in halo(e):
            c.wait_send()

    def share_done(s, sem):
        pltpu.make_async_copy(GB.at[s], GB.at[s], sem.at[s]).wait()

    def run(up):
        order = tuple(range(box)) if up else tuple(reversed(range(box)))
        close, distant = order[:-2], order[-2:]
        behind = [k for k, d in enumerate(DIRS) if d[0] == (-1 if up else 1)]
        ahead = [k for k in range(len(DIRS)) if k not in behind]
        faraway = (px + 2, px + 3) if up else (0, 1)

        def opening(derive, close, distant):
            for k in ahead:
                for c in pieces[k][0] + pieces[k][1]:
                    c.wait_recv()
            derive(close)

            def rest():
                for k in behind:
                    for c in pieces[k][0] + pieces[k][1]:
                        c.wait_recv()
                derive(distant)

            return rest

        def lift(e, tables, slots):
            for p in slots:
                table = tables[0 if p < 2 else 1 if p < 2 + px else 2]
                lifted = jnp.take_along_axis(table, AGX[p], axis=1, mode="promise_in_bounds")
                FIX[p] = CUR[e, 0, p] + lifted

        def receive(e):
            final = isinstance(e, int)
            share_done(e - 1, gs)
            landed = rings(e, 1) if final else halo(e)
            late_faces = [FACES.index((-1 if up else 1, 0))]
            late_corners = [k for k, d in enumerate(CORNERS) if d[0] == (-1 if up else 1)]
            slow = late_faces if final else late_faces + [len(FACES) + late_faces[0]] + [len(FACES) + 2 + k for k in late_corners]
            for k in range(len(landed)):
                if k not in slow:
                    landed[k].wait_recv()
            share_done(e - 1, gr)
            total = YB[e - 1, me_w]
            for k in range(len(pairs)):
                total = total + GB[e - 1, k]
            tables = [jnp.broadcast_to(total[k : k + 1], (2 * cy, tile)) for k in range(3)]
            if not final:
                unpack(e, [k for k in range(len(CORNERS)) if k not in late_corners])
            lift(e, tables, [p for p in range(px + 4) if p not in faraway])

            def rest():
                for k in slow:
                    landed[k].wait_recv()
                if not final:
                    unpack(e, late_corners)
                lift(e, tables, faraway)

            return rest

        def begin_box(read, boxes, acc):
            for b, applied in operate(read, boxes, True):
                h = [COEF[first_rhs + c, b + 1] - applied[c] for c in range(phases)]
                for c in range(phases):
                    H[c, b] = h[c]
                out = product(b, scaled(b, h), ring_rows if b in inner else near_rows)
                for c in range(phases):
                    W1[c, b + 1] = out[c]
                if acc is not None and b in inner:
                    acc = gather(acc, b - 1, h[0])
            return acc

        def sweep(s, first):
            read = current(s)
            def improve(boxes):
                for b, applied in operate(lambda c, idx: W1[c, idx], boxes):
                    q = scaled(b, [H[c, b] - applied[c] for c in range(phases)])
                    out = product(b, q, near_rows if b in inner else None)
                    n = 2 * cy if b in inner else cy
                    for c in range(phases):
                        W2[c, b + 1, :n] = W1[c, b + 1, :n] + out[c]

            rest = opening(derive, close, distant) if first else receive(s)
            acc = begin_box(read, close, None if first else jnp.zeros((aggs, tile), F32))
            improve(order[:0])
            rest()
            acc = begin_box(read, distant, acc)
            if not first:
                for c in solve_coarse(s, acc):
                    c.start()
            improve(order[0:])
            done = []
            for b, applied in operate(lambda c, idx: W2[c, idx], order[1:-1]):
                done.append((b, product(b, scaled(b, [H[c, b] - applied[c] for c in range(phases)]), None)))
            for b, out in done:
                for c in range(phases):
                    CUR[s + 1, c, b + 1, :cy] = read(c, b + 1)[:cy] + (W2[c, b + 1, :cy] + out[c])
            first_face = [1, 0, 2, 3] if up else [0, 1, 2, 3]

            def send_all():
                ring = rings(s + 1, 3)
                for k in first_face:
                    ring[k].start()
                pack(s + 1)
                more = extras(s + 1)
                turn = [1, 4, 5, 0, 2, 3] if up else [0, 2, 3, 1, 4, 5]
                for k in turn:
                    more[k].start()

            def send_last():
                ring = rings(s + 1, 1)
                for k in first_face:
                    ring[k].start()

            if first:
                send_all()
            else:
                pl.when(s + 1 < SWEEPS)(send_all)
                pl.when(s + 1 == SWEEPS)(send_last)
            drain(s)
            if first:
                for c in coef + thin + aggregates:
                    c.wait_send()
                for c in aggregates:
                    c.wait_recv()

        def later(s, carry):
            sweep(s, False)
            return carry

        sweep(0, True)
        lax.fori_loop(1, SWEEPS, later, 0)
        rest = receive(SWEEPS)
        last = current(SWEEPS)
        for c in range(phases):
            for p in range(px):
                out_it[c, p] = last(c, p + 2)[:cy]

        def finish(boxes):
            for b, applied in operate(last, boxes):
                for c in range(phases):
                    out_res[c, b - 1] = COEF[first_rhs + c, b + 1, 0:cy] - applied[c][:cy]

        finish(close[1:])
        rest()
        finish(distant[:1])
        for c in rings(SWEEPS, 1):
            c.wait_send()

    for p in range(px + 4):
        FIX[p] = CUR[0, 0, p]

    @pl.when(odd == 1)
    def _():
        run(True)

    @pl.when(odd == 0)
    def _():
        run(False)


def hand_over(iterate, residual, out_it, out_res, sem):
    moves = [
        pltpu.make_async_copy(iterate, out_it, sem.at[0]),
        pltpu.make_async_copy(residual, out_res, sem.at[1]),
    ]
    for c in moves:
        c.start()
    for c in moves:
        c.wait()


def solution(mesh):
    nw, nn = mesh.shape["wide"], mesh.shape["narrow"]

    def per_device(rhs, start, trans, accum, coupling, well_cells, well_index, agg_map, tile_factors, coarse_inverse):
        phases, px, cy, tile = rhs.shape
        box = px + 2
        aggs = coarse_inverse.shape[0]
        conn = well_cells.size
        nch = 4 + phases * phases + phases
        vmem = pl.BlockSpec(memory_space=pltpu.VMEM)
        hbm = pl.BlockSpec(memory_space=pl.ANY)
        shape = jax.ShapeDtypeStruct(rhs.shape, F32)
        ring = (2 * cy, tile)
        dma = pltpu.SemaphoreType.DMA
        call = pl.pallas_call(
            functools.partial(body, nw, nn),
            out_shape=(pltpu.VMEM(rhs.shape, F32), pltpu.VMEM(rhs.shape, F32)),
            in_specs=[hbm] * 10,
            out_specs=(vmem, vmem),
            scratch_shapes=[
                pltpu.VMEM((nch, px + 4) + ring, F32),
                pltpu.VMEM((SWEEPS + 1, phases, px + 4) + ring, F32),
                pltpu.VMEM((px + 4,) + ring, F32),
                pltpu.VMEM((phases, px + 4) + ring, F32),
                pltpu.VMEM((phases, px + 4) + ring, F32),
                pltpu.VMEM((phases, box) + ring, F32),
                pltpu.VMEM((4 + 2 * phases, box) + ring, F32),
                pltpu.VMEM(tile_factors.shape, tile_factors.dtype),
                pltpu.VMEM((box, (cy // 2 + 2) * tile, 2 * tile), tile_factors.dtype),
                pltpu.VMEM(coarse_inverse.shape, F32),
                pltpu.VMEM((px * cy, tile), jnp.int32),
                pltpu.VMEM((px + 4,) + ring, jnp.int32),
                pltpu.VMEM(accum.shape, F32),
                pltpu.VMEM((1, conn), jnp.int32),
                pltpu.VMEM((1, conn), F32),
                pltpu.VMEM((SWEEPS, nw * nn - 1, 3, tile), F32),
                pltpu.VMEM((SWEEPS, nw, 3, tile), F32),
                pltpu.VMEM((cy, tile), F32),
                pltpu.VMEM((px, 1, tile), F32),
                pltpu.VMEM((SWEEPS, 2, 2, cy, tile), F32),
                pltpu.VMEM((SWEEPS, len(CORNERS), 2 * phases + 2, tile), F32),
                pltpu.VMEM((SWEEPS, len(CORNERS), 2 * phases + 2, tile), F32),
                dma((10,)),
                dma((SWEEPS + 1, len(DIRS) + 2)),
                dma((SWEEPS + 1, len(DIRS) + 2)),
                dma((22,)),
                dma((22,)),
                dma((SWEEPS,)),
                dma((SWEEPS,)),
                dma((len(DIRS),)),
                dma((len(DIRS),)),
                dma((2,)),
                dma((2,)),
                pltpu.SemaphoreType.REGULAR,
                pltpu.SemaphoreType.REGULAR((max(nw, nn),)),
            ],
            compiler_params=pltpu.CompilerParams(collective_id=0, has_side_effects=True),
            name="schwarz",
        )
        held = call(
            rhs, start, trans, accum,
            coupling.reshape((phases * phases,) + accum.shape),
            well_cells.reshape(1, -1), well_index.reshape(1, -1),
            agg_map.reshape(px * cy, tile), tile_factors, coarse_inverse)
        held = [pltpu.with_memory_space_constraint(x, pltpu.VMEM) for x in held]
        return pl.pallas_call(
            hand_over, out_shape=(shape, shape), in_specs=[vmem, vmem], out_specs=(hbm, hbm),
            scratch_shapes=[dma((2,))], name="hand_over",
        )(*held)

    return jax.shard_map(
        per_device,
        mesh=mesh,
        in_specs=(
            P(None, "wide", "narrow", None),
            P(None, "wide", "narrow", None),
            P(None, "wide", "narrow", None),
            P("wide", "narrow", None),
            P(None, None, "wide", "narrow", None),
            P("wide", "narrow", None),
            P("wide", "narrow", None),
            P("wide", "narrow", None),
            P("wide", "narrow", None, None),
            P(("wide", "narrow"), None),
        ),
        out_specs=(P(None, "wide", "narrow", None), P(None, "wide", "narrow", None)),
        check_vma=False,
    )
```

```python
import functools

import jax
import jax.numpy as jnp
from jax import lax
from jax.experimental import pallas as pl
from jax.experimental.pallas import tpu as pltpu
from jax.sharding import PartitionSpec as P

SWEEPS = 3
HIGHEST = lax.Precision.HIGHEST
NT = (((1,), (1,)), ((), ()))
F32 = jnp.float32

DIRS = ((-1, 0), (1, 0), (0, -1), (0, 1), (-1, -1), (-1, 1), (1, -1), (1, 1))
FACES, CORNERS = DIRS[:4], DIRS[4:]
UP_FIRST = (1, 6, 7, 2, 3, 0, 4, 5)
DOWN_FIRST = (0, 4, 5, 2, 3, 1, 6, 7)
TX, ACW, TY, TZ = range(4)


def slot(t, cy):
    if t < cy:
        return t + 2
    return t + 2 if t < cy + 2 else t - cy - 2


def mirror(me, k, n):
    out, bit = 0, 1
    while bit < n:
        own = lax.rem(me // bit, 2)
        out = out + bit * (1 - own if (k // bit) % 2 else own)
        bit *= 2
    return out


def halo_piece(d, px, cy, depth_x, depth_y):
    dx, dy = d
    if dx == 0:
        sp, dp, npair = 2, 2, px
    elif dx > 0:
        sp, dp, npair = 2 + px - depth_x, 2 - depth_x, depth_x
    else:
        sp, dp, npair = 2, 2 + px, depth_x
    if dy == 0:
        sr, dr, nrow = 0, 0, cy
    elif dy > 0:
        sr, dr, nrow = cy - depth_y, 2 * cy - depth_y, depth_y
    else:
        sr, dr, nrow = 0, cy, depth_y
    return (pl.ds(sp, npair), pl.ds(sr, nrow)), (pl.ds(dp, npair), pl.ds(dr, nrow))


def body(
    nw, nn,
    rhs, start, trans, accum, coupling, cells, widx, agg, tiles, cinv,
    out_it, out_res,
    COEF, CUR, FIX, W1, W2, H, DER, TF, WT, CI, AG, AGX, ACC, CELLS, WIDX, GB, YB, XT, YT, SECOND, PACK, LAND,
    loc, hs, hr, cs, cr, gs, gr, is_, ir, ts, tr, near, far,
):
    phases = rhs.shape[0]
    px, cy, tile = accum.shape
    box = px + 2
    half = tile // 2
    aggs = CI.shape[0]
    me_w, me_n = lax.axis_index("wide"), lax.axis_index("narrow")

    def dev(dw, dn):
        return {"wide": lax.rem(me_w + dw + nw, nw), "narrow": lax.rem(me_n + dn + nn, nn)}

    own = pl.ds(2, px)
    top = pl.ds(0, cy)
    nch = COEF.shape[0]
    first_rhs = nch - phases
    copies = [
        (cells, CELLS),
        (widx, WIDX),
        (accum, ACC),
        (trans.at[pl.ds(0, 1)], COEF.at[pl.ds(TX, 1), own, top]),
        (start, CUR.at[0, :, own, top]),
        (coupling, COEF.at[pl.ds(4, phases * phases), own, top]),
        (rhs, COEF.at[pl.ds(first_rhs, phases), own, top]),
        (agg, AG),
        (cinv, CI),
        (tiles, TF),
        (trans.at[pl.ds(1, 2)], COEF.at[pl.ds(TY, 2), own, top]),
    ]
    local = [pltpu.make_async_copy(s, d, loc.at[k]) for k, (s, d) in enumerate(copies)]
    for c in local:
        c.start()

    pairs = [(a, c) for a in reversed(range(nw)) for c in reversed(range(nn)) if a or c]
    mirror_w = [mirror(me_w, a, nw) for a in range(nw)]
    mirror_n = [mirror(me_n, c, nn) for c in range(nn)]

    def signal(sem, d):
        pl.semaphore_signal(sem, inc=1, device_id=dev(*d), device_id_type=pl.DeviceIdType.MESH)

    barrier = pltpu.get_barrier_semaphore()
    for p in range(px + 4):
        AGX[p] = jnp.zeros((2 * cy, tile), jnp.int32)
    for d in DIRS:
        signal(barrier, d)

    def remote(src, dst, ss, rs, d):
        return pltpu.make_async_remote_copy(
            src_ref=src, dst_ref=dst, send_sem=ss, recv_sem=rs,
            device_id=dev(*d), device_id_type=pl.DeviceIdType.MESH,
        )

    def copy(src, dst, e, k, d):
        return remote(src, dst, hs.at[e, k], hr.at[e, k], d)

    def rings(e, depth_y):
        out = []
        for k, d in enumerate(FACES):
            src, dst = halo_piece(d, px, cy, 1, depth_y)
            out.append(copy(CUR.at[(e, slice(None)) + src], CUR.at[(e, slice(None)) + dst], e, k, d))
        return out

    def extras(e):
        n = len(FACES)
        out = [copy(SECOND.at[e, k], CUR.at[e, pl.ds(0, 2), 0 if d[0] > 0 else px + 3, top], e, n + k, d)
               for k, d in enumerate(FACES[:2])]
        return out + [copy(PACK.at[e, k], LAND.at[e, k], e, n + 2 + k, d) for k, d in enumerate(CORNERS)]

    def halo(e):
        return rings(e, 3) + extras(e)

    def pack(e):
        lower = lax.broadcasted_iota(jnp.int32, (cy, tile), 1) < half
        for k, d in enumerate(FACES[:2]):
            p = px if d[0] > 0 else 3
            one, two = CUR[e, 1, p, :cy], pltpu.roll(CUR[e, 2, p, :cy], half, 1)
            SECOND[e, k, 0] = CUR[e, 0, p, :cy]
            SECOND[e, k, 1] = jnp.where(lower, two, one) if d[0] > 0 else jnp.where(lower, one, two)
        for k, d in enumerate(CORNERS):
            p = px + 1 if d[0] > 0 else 2
            y0, y1 = (cy - 1, cy - 2) if d[1] > 0 else (0, 1)
            for c in range(phases):
                PACK[e, k, pl.ds(2 * c, 1)] = CUR[e, c, p, pl.ds(y0, 1)]
                PACK[e, k, pl.ds(2 * c + 1, 1)] = CUR[e, c, p, pl.ds(y1, 1)]
            for c in range(2):
                PACK[e, k, pl.ds(2 * phases + c, 1)] = SECOND[e, 1 if d[0] > 0 else 0, c, pl.ds(y0, 1)]

    def unpack(e, corners):
        for k in corners:
            d = CORNERS[k]
            p, q = (1, 0) if d[0] > 0 else (px + 2, px + 3)
            y0, y1 = (2 * cy - 1, 2 * cy - 2) if d[1] > 0 else (cy, cy + 1)
            for c in range(phases):
                CUR[e, c, p, pl.ds(y0, 1)] = LAND[e, k, pl.ds(2 * c, 1)]
                CUR[e, c, p, pl.ds(y1, 1)] = LAND[e, k, pl.ds(2 * c + 1, 1)]
            for c in range(2):
                CUR[e, c, q, pl.ds(y0, 1)] = LAND[e, k, pl.ds(2 * phases + c, 1)]

    coef, bulk, late = [], ([], []), ([], [])

    def send_coef(channels, src, dst, d):
        k = len(coef)
        coef.append(remote(COEF.at[(channels,) + src], COEF.at[(channels,) + dst], cs.at[k], cr.at[k], d))
        return coef[-1]

    pieces = []
    for d in DIRS:
        corner = d[0] != 0 and d[1] != 0
        depth_y = 1 if d[0] else 2
        src, dst = halo_piece(d, px, cy, 1, depth_y)
        skip = ACW if corner and d[0] > 0 else TX
        main = [send_coef(pl.ds(skip, nch - skip), src, dst, d)]
        rest = []
        if corner and d[0] > 0:
            src2, dst2 = halo_piece(d, px, cy, 2, 2)
            rest.append(send_coef(pl.ds(TX, 1), src2, dst2, d))
        elif d[0] > 0:
            rest.append(send_coef(pl.ds(TX, 1), (pl.ds(px, 1), src[1]), (pl.ds(0, 1), dst[1]), d))
        if d[1] > 0:
            rest.append(send_coef(pl.ds(TY, 1), (src[0], pl.ds(cy - depth_y - 1, 1)), (dst[0], pl.ds(2 * cy - depth_y - 1, 1)), d))
        pieces.append((main, rest))
    thin = [
        remote(COEF.at[TX, px + 1, top], XT, ts.at[0], tr.at[0], (1, 0)),
        remote(COEF.at[TY, own, pl.ds(cy - 1, 1)], YT, ts.at[1], tr.at[1], (0, 1)),
    ]
    for k in UP_FIRST:
        bulk[0].extend(pieces[k][0])
        late[0].extend(pieces[k][1])
    for k in DOWN_FIRST:
        bulk[1].extend(pieces[k][0])
        late[1].extend(pieces[k][1])

    aggregates = []
    for k, d in enumerate(DIRS):
        src, dst = halo_piece(d, px, cy, 2, 2 if d[0] else 3)
        aggregates.append(remote(AGX.at[src], AGX.at[dst], is_.at[k], ir.at[k], d))
    odd = lax.rem(me_w, 2)

    def start_all(first, second):
        @pl.when(odd == 1)
        def _():
            for c in first:
                c.start()

        @pl.when(odd == 0)
        def _():
            for c in second:
                c.start()

    local[4].wait()
    pack(0)
    pl.semaphore_wait(barrier, len(DIRS))
    for d in DIRS:
        signal(near, d)
    begin = halo(0)
    for c in begin:
        c.start()
    local[3].wait()
    local[10].wait()
    for c in thin:
        c.start()
    for c in (local[5], local[6]):
        c.wait()
    conn = cells.shape[-1]
    for c in local[:3]:
        c.wait()
    cell_row = CELLS[...]
    rows_own = px * cy
    hit_r = lax.broadcasted_iota(jnp.int32, (rows_own, conn), 0) == cell_row // tile
    hit_l = lax.broadcasted_iota(jnp.int32, (tile, conn), 0) == cell_row % tile
    left = jnp.where(hit_r, jnp.broadcast_to(WIDX[...], (rows_own, conn)), 0.0)
    right = jnp.where(hit_l, 1.0, 0.0)
    wells = lax.dot_general(left, right, NT, precision=HIGHEST, preferred_element_type=F32)
    COEF[ACW, 2 : 2 + px, 0:cy, :] = ACC[...] + wells.reshape(px, cy, tile)
    start_all(*bulk)
    start_all(*late)
    local[7].wait()
    AGX[2 : 2 + px, 0:cy] = (AG[...] + me_n * aggs).reshape(px, cy, tile)
    for c in aggregates:
        c.start()

    lane = lax.broadcasted_iota(jnp.int32, (2 * cy, tile), 1)
    low = lane < half
    roll = pltpu.roll

    zero16 = jnp.zeros((2 * cy, tile), F32)
    for c in range(phases):
        for w in (W1, W2):
            w[c, 0] = zero16
            w[c, box + 1] = zero16
        W2[c, 1] = zero16
        W2[c, box] = zero16
    rounds, reach = [], 2
    while reach < max(nw // 2, nn // 2):
        ws = (0,) if reach >= nw // 2 else (-reach, 0, reach)
        ns = (0,) if reach >= nn // 2 else (-reach, 0, reach)
        rounds.append([(a, c) for a in ws for c in ns if a or c])
        reach *= 2

    def join(opening):
        for k, group in enumerate(rounds):
            if opening == (k == 0):
                for d in group:
                    signal(far.at[k], d)
            if not opening:
                pl.semaphore_wait(far.at[k], len(group))

    pl.semaphore_wait(near, len(DIRS))
    join(True)
    local[9].wait()
    half_y = cy // 2
    for b in range(box):
        for t in range(cy + 4):
            if t < cy:
                kb, nb = t % half_y, t // half_y
            else:
                kb, nb = half_y + (t != cy and t != cy + 3), (t - cy) // 2
            WT[b, kb * tile : (kb + 1) * tile, nb * tile : (nb + 1) * tile] = TF[b, slot(t, cy)].T
    join(False)
    agg_iota = lax.broadcasted_iota(jnp.int32, (aggs, tile), 0)

    def gather(acc, p, h):
        for y in range(cy):
            ids = AG[pl.ds(p * cy + y, 1), :]
            acc = acc + jnp.where(agg_iota == ids, h[y : y + 1], 0.0)
        return acc

    def solve_coarse(s, acc):
        sums = jnp.broadcast_to(jnp.sum(acc, axis=1, keepdims=True), (aggs, tile))
        for g in range(nw):
            y = jnp.sum(CI[:, g * tile : (g + 1) * tile] * sums, axis=0, keepdims=True)
            for k in range(3):
                YB[s, (g + 1 - k) % nw, k : k + 1] = y
        return [
            pltpu.make_async_remote_copy(
                src_ref=YB.at[s, mirror_w[a]], dst_ref=GB.at[s, k], send_sem=gs.at[s], recv_sem=gr.at[s],
                device_id={"wide": mirror_w[a], "narrow": mirror_n[c]}, device_id_type=pl.DeviceIdType.MESH)
            for k, (a, c) in enumerate(pairs)]

    local[8].wait()
    begin = halo(0)
    for c in begin + thin:
        c.wait_recv()
    unpack(0, range(len(CORNERS)))
    acc = jnp.zeros((aggs, tile), F32)
    for p in range(px):
        idx = p + 2
        v, e, w = CUR[0, 0, idx], CUR[0, 0, idx + 1, :cy], CUR[0, 0, idx - 1, :cy]
        o = v[:cy]
        lo = low[:cy]
        tx, ty, tz = (COEF[k, idx, :cy] for k in (TX, TY, TZ))
        txw = jnp.where(lo, roll(XT[...] if p == 0 else COEF[TX, idx - 1, :cy], half, 1), roll(tx, half, 1))
        tys = jnp.where(lax.broadcasted_iota(jnp.int32, (cy, tile), 0) == 0, YT[p], roll(ty, 1, 0))
        tz = jnp.where(lane[:cy] % half < half - 1, tz, 0.0)
        tzd = roll(tz, 1, 1)
        turned = roll(o, half, 1)
        total = (COEF[ACW, idx, :cy] + (tx + txw + ty + tys + tz + tzd) + COEF[4, idx, :cy]) * o
        for k in range(1, phases):
            total = total + COEF[4 + k, idx, :cy] * CUR[0, k, idx, :cy]
        inflow = tx * jnp.where(lo, turned, roll(e, half, 1)) + txw * jnp.where(lo, roll(w, half, 1), turned)
        inflow = inflow + ty * roll(v, 2 * cy - 1, 0)[:cy] + tys * roll(v, 1, 0)[:cy]
        inflow = inflow + tz * roll(o, tile - 1, 1) + tzd * roll(o, 1, 1)
        acc = gather(acc, p, COEF[first_rhs, idx, :cy] - (total - inflow))
    for c in solve_coarse(0, acc):
        c.start()
    def derive(boxes):
        for b in boxes:
            tx = COEF[TX, b + 1]
            txw = jnp.where(low, roll(COEF[TX, b], half, 1), roll(tx, half, 1))
            ty = COEF[TY, b + 1]
            tys = roll(ty, 1, 0)
            tz = jnp.where(lane % half < half - 1, COEF[TZ, b + 1], 0.0)
            tzd = roll(tz, 1, 1)
            centre = COEF[ACW, b + 1] + (tx + txw + ty + tys + tz + tzd)
            DER[0, b] = txw
            DER[1, b] = tys
            DER[2, b] = tz
            DER[3, b] = tzd
            for c in range(phases):
                diag = centre + COEF[4 + c * phases + c, b + 1]
                DER[4 + c, b] = diag
                DER[4 + phases + c, b] = 1.0 / diag

    def operate(read, boxes, packed=False):
        swapped = {}

        def swap(c, idx):
            if packed and c == 2 and idx in (0, px + 3):
                return read(1, idx)
            if (c, idx) not in swapped:
                swapped[c, idx] = roll(read(c, idx), half, 1)
            return swapped[c, idx]

        for b in boxes:
            values = [read(c, b + 1) for c in range(phases)]
            result = []
            for c in range(phases):
                v = values[c]
                east = jnp.where(low, swap(c, b + 1), swap(c, b + 2))
                west = jnp.where(low, swap(c, b), swap(c, b + 1))
                total = DER[4 + c, b] * v
                for o in range(phases):
                    if o != c:
                        total = total + COEF[4 + c * phases + o, b + 1] * values[o]
                inflow = COEF[TX, b + 1] * east + DER[0, b] * west
                inflow = inflow + COEF[TY, b + 1] * roll(v, 2 * cy - 1, 0)
                inflow = inflow + DER[1, b] * roll(v, 1, 0)
                inflow = inflow + DER[2, b] * roll(v, tile - 1, 1)
                inflow = inflow + DER[3, b] * roll(v, 1, 1)
                result.append(total - inflow)
            yield b, result

    row = lax.broadcasted_iota(jnp.int32, (2 * cy, tile), 0)
    upper_half = ((row >= half_y) & (row < cy)) | (row >= 2 * cy - 2)
    own_blocks = [(row < cy) & (row % half_y == j) for j in range(half_y)]
    near_rows = ((row == cy) | (row == 2 * cy - 1),)
    ring_rows = near_rows + ((row == cy + 1) | (row == 2 * cy - 2),)

    def product(b, q, extra):
        n = cy if extra is None else 2 * cy
        blocks = own_blocks + list(extra or ())
        stack = jnp.concatenate([v[:n] for v in q], axis=0)
        masks = [jnp.concatenate([m[:n]] * phases, axis=0) for m in blocks]
        lhs = jnp.concatenate([jnp.where(m, stack, 0.0) for m in masks], axis=1).astype(jnp.bfloat16)
        out = jnp.dot(lhs, WT[b, : len(blocks) * tile, :], preferred_element_type=F32)
        return [jnp.where(upper_half[:n], out[c * n : (c + 1) * n, tile:], out[c * n : (c + 1) * n, :tile])
                for c in range(phases)]

    inner = range(1, box - 1)

    def scaled(b, h):
        return [DER[4 + phases + c, b] * h[c] for c in range(phases)]

    def current(e):
        return lambda c, idx: FIX[idx] if c == 0 else CUR[e, c, idx]

    def drain(e):
        for c in halo(e):
            c.wait_send()

    def share_done(s, sem):
        pltpu.make_async_copy(GB.at[s], GB.at[s], sem.at[s]).wait()

    def run(up):
        order = tuple(range(box)) if up else tuple(reversed(range(box)))
        close, distant = order[:-2], order[-2:]
        behind = [k for k, d in enumerate(DIRS) if d[0] == (-1 if up else 1)]
        ahead = [k for k in range(len(DIRS)) if k not in behind]
        faraway = (px + 2, px + 3) if up else (0, 1)

        def opening(derive, close, distant):
            for k in ahead:
                for c in pieces[k][0] + pieces[k][1]:
                    c.wait_recv()
            derive(close)

            def rest():
                for k in behind:
                    for c in pieces[k][0] + pieces[k][1]:
                        c.wait_recv()
                derive(distant)

            return rest

        def lifts(tables, slots):
            out = []
            for p in slots:
                table = tables[0 if p < 2 else 1 if p < 2 + px else 2]
                out.append((p, jnp.take_along_axis(table, AGX[p], axis=1, mode="promise_in_bounds")))
            return out

        def lift(e, found):
            for p, lifted in found:
                FIX[p] = CUR[e, 0, p] + lifted

        def receive(e):
            final = isinstance(e, int)
            share_done(e - 1, gs)
            landed = rings(e, 1) if final else halo(e)
            late_faces = [FACES.index((-1 if up else 1, 0))]
            late_corners = [k for k, d in enumerate(CORNERS) if d[0] == (-1 if up else 1)]
            slow = late_faces if final else late_faces + [len(FACES) + late_faces[0]] + [len(FACES) + 2 + k for k in late_corners]
            for k in range(len(landed)):
                if k not in slow:
                    landed[k].wait_recv()
            share_done(e - 1, gr)
            parts = [YB[e - 1, me_w]] + [GB[e - 1, k] for k in range(len(pairs))]
            while len(parts) > 1:
                parts = [sum(parts[k : k + 2][1:], parts[k]) for k in range(0, len(parts), 2)]
            total = parts[0]
            tables = [jnp.broadcast_to(total[k : k + 1], (2 * cy, tile)) for k in range(3)]
            if not final:
                unpack(e, [k for k in range(len(CORNERS)) if k not in late_corners])
            lift(e, lifts(tables, [p for p in range(px + 4) if p not in faraway]))
            ready = lifts(tables, faraway)

            def rest():
                for k in slow:
                    landed[k].wait_recv()
                if not final:
                    unpack(e, late_corners)
                lift(e, ready)

            return rest

        def begin_box(read, boxes, acc):
            for b, applied in operate(read, boxes, True):
                h = [COEF[first_rhs + c, b + 1] - applied[c] for c in range(phases)]
                for c in range(phases):
                    H[c, b] = h[c]
                out = product(b, scaled(b, h), ring_rows if b in inner else near_rows)
                for c in range(phases):
                    W1[c, b + 1] = out[c]
                if acc is not None and b in inner:
                    acc = gather(acc, b - 1, h[0])
            return acc

        def sweep(s, first):
            read = current(s)
            def improve(boxes):
                for b, applied in operate(lambda c, idx: W1[c, idx], boxes):
                    q = scaled(b, [H[c, b] - applied[c] for c in range(phases)])
                    out = product(b, q, near_rows if b in inner else None)
                    n = 2 * cy if b in inner else cy
                    for c in range(phases):
                        W2[c, b + 1, :n] = W1[c, b + 1, :n] + out[c]

            rest = opening(derive, close, distant) if first else receive(s)
            acc = begin_box(read, close, None if first else jnp.zeros((aggs, tile), F32))
            improve(order[:0])
            rest()
            acc = begin_box(read, distant, acc)
            if not first:
                for c in solve_coarse(s, acc):
                    c.start()
            improve(order[0:])
            done = []
            for b, applied in operate(lambda c, idx: W2[c, idx], order[1:-1]):
                done.append((b, product(b, scaled(b, [H[c, b] - applied[c] for c in range(phases)]), None)))
            for b, out in done:
                for c in range(phases):
                    CUR[s + 1, c, b + 1, :cy] = read(c, b + 1)[:cy] + (W2[c, b + 1, :cy] + out[c])
            first_face = [1, 0, 2, 3] if up else [0, 1, 2, 3]

            def send_all():
                ring = rings(s + 1, 3)
                for k in first_face:
                    ring[k].start()
                pack(s + 1)
                more = extras(s + 1)
                turn = [1, 4, 5, 0, 2, 3] if up else [0, 2, 3, 1, 4, 5]
                for k in turn:
                    more[k].start()

            def send_last():
                ring = rings(s + 1, 1)
                for k in first_face:
                    ring[k].start()

            if first:
                send_all()
            else:
                pl.when(s + 1 < SWEEPS)(send_all)
                pl.when(s + 1 == SWEEPS)(send_last)
            drain(s)
            if first:
                for c in coef + thin + aggregates:
                    c.wait_send()
                for c in aggregates:
                    c.wait_recv()

        def later(s, carry):
            sweep(s, False)
            return carry

        sweep(0, True)
        lax.fori_loop(1, SWEEPS, later, 0)
        rest = receive(SWEEPS)
        last = current(SWEEPS)
        for c in range(phases):
            for p in range(px):
                out_it[c, p] = last(c, p + 2)[:cy]

        def finish(boxes):
            for b, applied in operate(last, boxes):
                for c in range(phases):
                    out_res[c, b - 1] = COEF[first_rhs + c, b + 1, 0:cy] - applied[c][:cy]

        finish(close[1:])
        rest()
        finish(distant[:1])
        for c in rings(SWEEPS, 1):
            c.wait_send()

    for p in range(px + 4):
        FIX[p] = CUR[0, 0, p]

    @pl.when(odd == 1)
    def _():
        run(True)

    @pl.when(odd == 0)
    def _():
        run(False)


def hand_over(iterate, residual, out_it, out_res, sem):
    moves = [
        pltpu.make_async_copy(iterate, out_it, sem.at[0]),
        pltpu.make_async_copy(residual, out_res, sem.at[1]),
    ]
    for c in moves:
        c.start()
    for c in moves:
        c.wait()


def solution(mesh):
    nw, nn = mesh.shape["wide"], mesh.shape["narrow"]

    def per_device(rhs, start, trans, accum, coupling, well_cells, well_index, agg_map, tile_factors, coarse_inverse):
        phases, px, cy, tile = rhs.shape
        box = px + 2
        aggs = coarse_inverse.shape[0]
        conn = well_cells.size
        nch = 4 + phases * phases + phases
        vmem = pl.BlockSpec(memory_space=pltpu.VMEM)
        hbm = pl.BlockSpec(memory_space=pl.ANY)
        shape = jax.ShapeDtypeStruct(rhs.shape, F32)
        ring = (2 * cy, tile)
        dma = pltpu.SemaphoreType.DMA
        call = pl.pallas_call(
            functools.partial(body, nw, nn),
            out_shape=(pltpu.VMEM(rhs.shape, F32), pltpu.VMEM(rhs.shape, F32)),
            in_specs=[hbm] * 10,
            out_specs=(vmem, vmem),
            scratch_shapes=[
                pltpu.VMEM((nch, px + 4) + ring, F32),
                pltpu.VMEM((SWEEPS + 1, phases, px + 4) + ring, F32),
                pltpu.VMEM((px + 4,) + ring, F32),
                pltpu.VMEM((phases, px + 4) + ring, F32),
                pltpu.VMEM((phases, px + 4) + ring, F32),
                pltpu.VMEM((phases, box) + ring, F32),
                pltpu.VMEM((4 + 2 * phases, box) + ring, F32),
                pltpu.VMEM(tile_factors.shape, tile_factors.dtype),
                pltpu.VMEM((box, (cy // 2 + 2) * tile, 2 * tile), tile_factors.dtype),
                pltpu.VMEM(coarse_inverse.shape, F32),
                pltpu.VMEM((px * cy, tile), jnp.int32),
                pltpu.VMEM((px + 4,) + ring, jnp.int32),
                pltpu.VMEM(accum.shape, F32),
                pltpu.VMEM((1, conn), jnp.int32),
                pltpu.VMEM((1, conn), F32),
                pltpu.VMEM((SWEEPS, nw * nn - 1, 3, tile), F32),
                pltpu.VMEM((SWEEPS, nw, 3, tile), F32),
                pltpu.VMEM((cy, tile), F32),
                pltpu.VMEM((px, 1, tile), F32),
                pltpu.VMEM((SWEEPS, 2, 2, cy, tile), F32),
                pltpu.VMEM((SWEEPS, len(CORNERS), 2 * phases + 2, tile), F32),
                pltpu.VMEM((SWEEPS, len(CORNERS), 2 * phases + 2, tile), F32),
                dma((11,)),
                dma((SWEEPS + 1, len(DIRS) + 2)),
                dma((SWEEPS + 1, len(DIRS) + 2)),
                dma((14,)),
                dma((14,)),
                dma((SWEEPS,)),
                dma((SWEEPS,)),
                dma((len(DIRS),)),
                dma((len(DIRS),)),
                dma((2,)),
                dma((2,)),
                pltpu.SemaphoreType.REGULAR,
                pltpu.SemaphoreType.REGULAR((max(nw, nn),)),
            ],
            compiler_params=pltpu.CompilerParams(collective_id=0, has_side_effects=True),
            name="schwarz",
        )
        held = call(
            rhs, start, trans, accum,
            coupling.reshape((phases * phases,) + accum.shape),
            well_cells.reshape(1, -1), well_index.reshape(1, -1),
            agg_map.reshape(px * cy, tile), tile_factors, coarse_inverse)
        held = [pltpu.with_memory_space_constraint(x, pltpu.VMEM) for x in held]
        return pl.pallas_call(
            hand_over, out_shape=(shape, shape), in_specs=[vmem, vmem], out_specs=(hbm, hbm),
            scratch_shapes=[dma((2,))], name="hand_over",
        )(*held)

    return jax.shard_map(
        per_device,
        mesh=mesh,
        in_specs=(
            P(None, "wide", "narrow", None),
            P(None, "wide", "narrow", None),
            P(None, "wide", "narrow", None),
            P("wide", "narrow", None),
            P(None, None, "wide", "narrow", None),
            P("wide", "narrow", None),
            P("wide", "narrow", None),
            P("wide", "narrow", None),
            P("wide", "narrow", None, None),
            P(("wide", "narrow"), None),
        ),
        out_specs=(P(None, "wide", "narrow", None), P(None, "wide", "narrow", None)),
        check_vma=False,
    )
```

```python
import functools

import jax
import jax.numpy as jnp
from jax import lax
from jax.experimental import pallas as pl
from jax.experimental.pallas import tpu as pltpu
from jax.sharding import PartitionSpec as P

SWEEPS = 3
HIGHEST = lax.Precision.HIGHEST
NT = (((1,), (1,)), ((), ()))
F32 = jnp.float32

DIRS = ((-1, 0), (1, 0), (0, -1), (0, 1), (-1, -1), (-1, 1), (1, -1), (1, 1))
FACES, CORNERS = DIRS[:4], DIRS[4:]
UP_FIRST = (1, 6, 7, 2, 3, 0, 4, 5)
DOWN_FIRST = (0, 4, 5, 2, 3, 1, 6, 7)
TX, ACW, TY, TZ = range(4)


def slot(t, cy):
    if t < cy:
        return t + 2
    return t + 2 if t < cy + 2 else t - cy - 2


def mirror(me, k, n):
    out, bit = 0, 1
    while bit < n:
        own = lax.rem(me // bit, 2)
        out = out + bit * (1 - own if (k // bit) % 2 else own)
        bit *= 2
    return out


def halo_piece(d, px, cy, depth_x, depth_y):
    dx, dy = d
    if dx == 0:
        sp, dp, npair = 2, 2, px
    elif dx > 0:
        sp, dp, npair = 2 + px - depth_x, 2 - depth_x, depth_x
    else:
        sp, dp, npair = 2, 2 + px, depth_x
    if dy == 0:
        sr, dr, nrow = 0, 0, cy
    elif dy > 0:
        sr, dr, nrow = cy - depth_y, 2 * cy - depth_y, depth_y
    else:
        sr, dr, nrow = 0, cy, depth_y
    return (pl.ds(sp, npair), pl.ds(sr, nrow)), (pl.ds(dp, npair), pl.ds(dr, nrow))


def body(
    nw, nn,
    rhs, start, trans, accum, coupling, cells, widx, agg, tiles, cinv,
    out_it, out_res,
    COEF, CUR, FIX, W1, W2, H, DER, TF, WT, CI, AG, AGX, ACC, CELLS, WIDX, GB, YB, XT, YT, SECOND, PACK, LAND,
    loc, hs, hr, cs, cr, gs, gr, is_, ir, ts, tr, near, far,
):
    phases = rhs.shape[0]
    px, cy, tile = accum.shape
    box = px + 2
    half = tile // 2
    aggs = CI.shape[0]
    me_w, me_n = lax.axis_index("wide"), lax.axis_index("narrow")

    def dev(dw, dn):
        return {"wide": lax.rem(me_w + dw + nw, nw), "narrow": lax.rem(me_n + dn + nn, nn)}

    own = pl.ds(2, px)
    top = pl.ds(0, cy)
    nch = COEF.shape[0]
    first_rhs = nch - phases
    copies = [
        (cells, CELLS),
        (widx, WIDX),
        (accum, ACC),
        (trans.at[pl.ds(0, 1)], COEF.at[pl.ds(TX, 1), own, top]),
        (start, CUR.at[0, :, own, top]),
        (coupling, COEF.at[pl.ds(4, phases * phases), own, top]),
        (rhs, COEF.at[pl.ds(first_rhs, phases), own, top]),
        (agg, AG),
        (cinv, CI),
        (tiles, TF),
        (trans.at[pl.ds(1, 2)], COEF.at[pl.ds(TY, 2), own, top]),
    ]
    local = [pltpu.make_async_copy(s, d, loc.at[k]) for k, (s, d) in enumerate(copies)]
    for c in local:
        c.start()

    pairs = [(a, c) for a in reversed(range(nw)) for c in reversed(range(nn)) if a or c]
    mirror_w = [mirror(me_w, a, nw) for a in range(nw)]
    mirror_n = [mirror(me_n, c, nn) for c in range(nn)]

    def signal(sem, d):
        pl.semaphore_signal(sem, inc=1, device_id=dev(*d), device_id_type=pl.DeviceIdType.MESH)

    barrier = pltpu.get_barrier_semaphore()
    for p in range(px + 4):
        AGX[p] = jnp.zeros((2 * cy, tile), jnp.int32)
    for d in DIRS:
        signal(barrier, d)

    def remote(src, dst, ss, rs, d):
        return pltpu.make_async_remote_copy(
            src_ref=src, dst_ref=dst, send_sem=ss, recv_sem=rs,
            device_id=dev(*d), device_id_type=pl.DeviceIdType.MESH,
        )

    def copy(src, dst, e, k, d):
        return remote(src, dst, hs.at[e, k], hr.at[e, k], d)

    def rings(e, depth_y):
        out = []
        for k, d in enumerate(FACES):
            src, dst = halo_piece(d, px, cy, 1, depth_y)
            out.append(copy(CUR.at[(e, slice(None)) + src], CUR.at[(e, slice(None)) + dst], e, k, d))
        return out

    def extras(e):
        n = len(FACES)
        out = [copy(SECOND.at[e, k], CUR.at[e, pl.ds(0, 2), 0 if d[0] > 0 else px + 3, top], e, n + k, d)
               for k, d in enumerate(FACES[:2])]
        return out + [copy(PACK.at[e, k], LAND.at[e, k], e, n + 2 + k, d) for k, d in enumerate(CORNERS)]

    def halo(e):
        return rings(e, 3) + extras(e)

    def pack(e):
        lower = lax.broadcasted_iota(jnp.int32, (cy, tile), 1) < half
        for k, d in enumerate(FACES[:2]):
            p = px if d[0] > 0 else 3
            one, two = CUR[e, 1, p, :cy], pltpu.roll(CUR[e, 2, p, :cy], half, 1)
            SECOND[e, k, 0] = CUR[e, 0, p, :cy]
            SECOND[e, k, 1] = jnp.where(lower, two, one) if d[0] > 0 else jnp.where(lower, one, two)
        for k, d in enumerate(CORNERS):
            p = px + 1 if d[0] > 0 else 2
            y0, y1 = (cy - 1, cy - 2) if d[1] > 0 else (0, 1)
            for c in range(phases):
                PACK[e, k, pl.ds(2 * c, 1)] = CUR[e, c, p, pl.ds(y0, 1)]
                PACK[e, k, pl.ds(2 * c + 1, 1)] = CUR[e, c, p, pl.ds(y1, 1)]
            for c in range(2):
                PACK[e, k, pl.ds(2 * phases + c, 1)] = SECOND[e, 1 if d[0] > 0 else 0, c, pl.ds(y0, 1)]

    def unpack(e, corners):
        for k in corners:
            d = CORNERS[k]
            p, q = (1, 0) if d[0] > 0 else (px + 2, px + 3)
            y0, y1 = (2 * cy - 1, 2 * cy - 2) if d[1] > 0 else (cy, cy + 1)
            for c in range(phases):
                CUR[e, c, p, pl.ds(y0, 1)] = LAND[e, k, pl.ds(2 * c, 1)]
                CUR[e, c, p, pl.ds(y1, 1)] = LAND[e, k, pl.ds(2 * c + 1, 1)]
            for c in range(2):
                CUR[e, c, q, pl.ds(y0, 1)] = LAND[e, k, pl.ds(2 * phases + c, 1)]

    coef, bulk, late = [], ([], []), ([], [])

    def send_coef(channels, src, dst, d):
        k = len(coef)
        coef.append(remote(COEF.at[(channels,) + src], COEF.at[(channels,) + dst], cs.at[k], cr.at[k], d))
        return coef[-1]

    pieces = []
    for d in DIRS:
        corner = d[0] != 0 and d[1] != 0
        depth_y = 1 if d[0] else 2
        src, dst = halo_piece(d, px, cy, 1, depth_y)
        skip = ACW if corner and d[0] > 0 else TX
        main = [send_coef(pl.ds(skip, nch - skip), src, dst, d)]
        rest = []
        if corner and d[0] > 0:
            src2, dst2 = halo_piece(d, px, cy, 2, 2)
            rest.append(send_coef(pl.ds(TX, 1), src2, dst2, d))
        elif d[0] > 0:
            rest.append(send_coef(pl.ds(TX, 1), (pl.ds(px, 1), src[1]), (pl.ds(0, 1), dst[1]), d))
        if d[1] > 0:
            rest.append(send_coef(pl.ds(TY, 1), (src[0], pl.ds(cy - depth_y - 1, 1)), (dst[0], pl.ds(2 * cy - depth_y - 1, 1)), d))
        pieces.append((main, rest))
    thin = [
        remote(COEF.at[TX, px + 1, top], XT, ts.at[0], tr.at[0], (1, 0)),
        remote(COEF.at[TY, own, pl.ds(cy - 1, 1)], YT, ts.at[1], tr.at[1], (0, 1)),
    ]
    for k in UP_FIRST:
        bulk[0].extend(pieces[k][0])
        late[0].extend(pieces[k][1])
    for k in DOWN_FIRST:
        bulk[1].extend(pieces[k][0])
        late[1].extend(pieces[k][1])

    aggregates = []
    for k, d in enumerate(DIRS):
        src, dst = halo_piece(d, px, cy, 2, 2 if d[0] else 3)
        aggregates.append(remote(AGX.at[src], AGX.at[dst], is_.at[k], ir.at[k], d))
    odd = lax.rem(me_w, 2)

    def start_all(first, second):
        @pl.when(odd == 1)
        def _():
            for c in first:
                c.start()

        @pl.when(odd == 0)
        def _():
            for c in second:
                c.start()

    local[4].wait()
    pl.semaphore_wait(barrier, len(DIRS))
    for d in DIRS:
        signal(near, d)
    begin = halo(0)
    for c in begin[:4]:
        c.start()
    pack(0)
    for c in begin[4:]:
        c.start()
    local[3].wait()
    local[10].wait()
    for c in thin:
        c.start()
    for c in (local[5], local[6]):
        c.wait()
    conn = cells.shape[-1]
    for c in local[:3]:
        c.wait()
    cell_row = CELLS[...]
    rows_own = px * cy
    hit_r = lax.broadcasted_iota(jnp.int32, (rows_own, conn), 0) == cell_row // tile
    hit_l = lax.broadcasted_iota(jnp.int32, (tile, conn), 0) == cell_row % tile
    left = jnp.where(hit_r, jnp.broadcast_to(WIDX[...], (rows_own, conn)), 0.0)
    right = jnp.where(hit_l, 1.0, 0.0)
    wells = lax.dot_general(left, right, NT, precision=HIGHEST, preferred_element_type=F32)
    COEF[ACW, 2 : 2 + px, 0:cy, :] = ACC[...] + wells.reshape(px, cy, tile)
    start_all(*bulk)
    start_all(*late)
    local[7].wait()
    AGX[2 : 2 + px, 0:cy] = (AG[...] + me_n * aggs).reshape(px, cy, tile)
    for c in aggregates:
        c.start()

    lane = lax.broadcasted_iota(jnp.int32, (2 * cy, tile), 1)
    low = lane < half
    roll = pltpu.roll

    zero16 = jnp.zeros((2 * cy, tile), F32)
    for c in range(phases):
        for w in (W1, W2):
            w[c, 0] = zero16
            w[c, box + 1] = zero16
        W2[c, 1] = zero16
        W2[c, box] = zero16
    rounds, reach = [], 2
    while reach < max(nw // 2, nn // 2):
        ws = (0,) if reach >= nw // 2 else (-reach, 0, reach)
        ns = (0,) if reach >= nn // 2 else (-reach, 0, reach)
        rounds.append([(a, c) for a in ws for c in ns if a or c])
        reach *= 2

    def join(opening):
        for k, group in enumerate(rounds):
            if opening == (k == 0):
                for d in group:
                    signal(far.at[k], d)
            if not opening:
                pl.semaphore_wait(far.at[k], len(group))

    pl.semaphore_wait(near, len(DIRS))
    join(True)
    local[9].wait()
    half_y = cy // 2
    for b in range(box):
        for t in range(cy + 4):
            if t < cy:
                kb, nb = t % half_y, t // half_y
            else:
                kb, nb = half_y + (t != cy and t != cy + 3), (t - cy) // 2
            WT[b, kb * tile : (kb + 1) * tile, nb * tile : (nb + 1) * tile] = TF[b, slot(t, cy)].T
    join(False)
    agg_iota = lax.broadcasted_iota(jnp.int32, (aggs, tile), 0)

    def gather(acc, p, h):
        for y in range(cy):
            ids = AG[pl.ds(p * cy + y, 1), :]
            acc = acc + jnp.where(agg_iota == ids, h[y : y + 1], 0.0)
        return acc

    def solve_coarse(s, acc):
        sums = jnp.broadcast_to(jnp.sum(acc, axis=1, keepdims=True), (aggs, tile))
        for g in range(nw):
            y = jnp.sum(CI[:, g * tile : (g + 1) * tile] * sums, axis=0, keepdims=True)
            for k in range(3):
                YB[s, (g + 1 - k) % nw, k : k + 1] = y
        return [
            pltpu.make_async_remote_copy(
                src_ref=YB.at[s, mirror_w[a]], dst_ref=GB.at[s, k], send_sem=gs.at[s], recv_sem=gr.at[s],
                device_id={"wide": mirror_w[a], "narrow": mirror_n[c]}, device_id_type=pl.DeviceIdType.MESH)
            for k, (a, c) in enumerate(pairs)]

    local[8].wait()
    begin = halo(0)
    for c in begin + thin:
        c.wait_recv()
    unpack(0, range(len(CORNERS)))
    acc = jnp.zeros((aggs, tile), F32)
    for p in range(px):
        idx = p + 2
        v, e, w = CUR[0, 0, idx], CUR[0, 0, idx + 1, :cy], CUR[0, 0, idx - 1, :cy]
        o = v[:cy]
        lo = low[:cy]
        tx, ty, tz = (COEF[k, idx, :cy] for k in (TX, TY, TZ))
        txw = jnp.where(lo, roll(XT[...] if p == 0 else COEF[TX, idx - 1, :cy], half, 1), roll(tx, half, 1))
        tys = jnp.where(lax.broadcasted_iota(jnp.int32, (cy, tile), 0) == 0, YT[p], roll(ty, 1, 0))
        tz = jnp.where(lane[:cy] % half < half - 1, tz, 0.0)
        tzd = roll(tz, 1, 1)
        turned = roll(o, half, 1)
        total = (COEF[ACW, idx, :cy] + (tx + txw + ty + tys + tz + tzd) + COEF[4, idx, :cy]) * o
        for k in range(1, phases):
            total = total + COEF[4 + k, idx, :cy] * CUR[0, k, idx, :cy]
        inflow = tx * jnp.where(lo, turned, roll(e, half, 1)) + txw * jnp.where(lo, roll(w, half, 1), turned)
        inflow = inflow + ty * roll(v, 2 * cy - 1, 0)[:cy] + tys * roll(v, 1, 0)[:cy]
        inflow = inflow + tz * roll(o, tile - 1, 1) + tzd * roll(o, 1, 1)
        acc = gather(acc, p, COEF[first_rhs, idx, :cy] - (total - inflow))
    for c in solve_coarse(0, acc):
        c.start()
    def derive(boxes):
        for b in boxes:
            tx = COEF[TX, b + 1]
            txw = jnp.where(low, roll(COEF[TX, b], half, 1), roll(tx, half, 1))
            ty = COEF[TY, b + 1]
            tys = roll(ty, 1, 0)
            tz = jnp.where(lane % half < half - 1, COEF[TZ, b + 1], 0.0)
            tzd = roll(tz, 1, 1)
            centre = COEF[ACW, b + 1] + (tx + txw + ty + tys + tz + tzd)
            DER[0, b] = txw
            DER[1, b] = tys
            DER[2, b] = tz
            DER[3, b] = tzd
            for c in range(phases):
                diag = centre + COEF[4 + c * phases + c, b + 1]
                DER[4 + c, b] = diag
                DER[4 + phases + c, b] = 1.0 / diag

    def operate(read, boxes, packed=False):
        swapped = {}

        def swap(c, idx):
            if packed and c == 2 and idx in (0, px + 3):
                return read(1, idx)
            if (c, idx) not in swapped:
                swapped[c, idx] = roll(read(c, idx), half, 1)
            return swapped[c, idx]

        for b in boxes:
            values = [read(c, b + 1) for c in range(phases)]
            result = []
            for c in range(phases):
                v = values[c]
                east = jnp.where(low, swap(c, b + 1), swap(c, b + 2))
                west = jnp.where(low, swap(c, b), swap(c, b + 1))
                total = DER[4 + c, b] * v
                for o in range(phases):
                    if o != c:
                        total = total + COEF[4 + c * phases + o, b + 1] * values[o]
                inflow = COEF[TX, b + 1] * east + DER[0, b] * west
                inflow = inflow + COEF[TY, b + 1] * roll(v, 2 * cy - 1, 0)
                inflow = inflow + DER[1, b] * roll(v, 1, 0)
                inflow = inflow + DER[2, b] * roll(v, tile - 1, 1)
                inflow = inflow + DER[3, b] * roll(v, 1, 1)
                result.append(total - inflow)
            yield b, result

    row = lax.broadcasted_iota(jnp.int32, (2 * cy, tile), 0)
    upper_half = ((row >= half_y) & (row < cy)) | (row >= 2 * cy - 2)
    own_blocks = [(row < cy) & (row % half_y == j) for j in range(half_y)]
    near_rows = ((row == cy) | (row == 2 * cy - 1),)
    ring_rows = near_rows + ((row == cy + 1) | (row == 2 * cy - 2),)

    def product(b, q, extra):
        n = cy if extra is None else 2 * cy
        blocks = own_blocks + list(extra or ())
        stack = jnp.concatenate([v[:n] for v in q], axis=0)
        masks = [jnp.concatenate([m[:n]] * phases, axis=0) for m in blocks]
        lhs = jnp.concatenate([jnp.where(m, stack, 0.0) for m in masks], axis=1).astype(jnp.bfloat16)
        out = jnp.dot(lhs, WT[b, : len(blocks) * tile, :], preferred_element_type=F32)
        return [jnp.where(upper_half[:n], out[c * n : (c + 1) * n, tile:], out[c * n : (c + 1) * n, :tile])
                for c in range(phases)]

    inner = range(1, box - 1)

    def scaled(b, h):
        return [DER[4 + phases + c, b] * h[c] for c in range(phases)]

    def current(e):
        return lambda c, idx: FIX[idx] if c == 0 else CUR[e, c, idx]

    def drain(e):
        for c in halo(e):
            c.wait_send()

    def share_done(s, sem):
        pltpu.make_async_copy(GB.at[s], GB.at[s], sem.at[s]).wait()

    def run(up):
        order = tuple(range(box)) if up else tuple(reversed(range(box)))
        close, distant = order[:-2], order[-2:]
        behind = [k for k, d in enumerate(DIRS) if d[0] == (-1 if up else 1)]
        ahead = [k for k in range(len(DIRS)) if k not in behind]
        faraway = (px + 2, px + 3) if up else (0, 1)

        def opening(derive, close, distant):
            for k in ahead:
                for c in pieces[k][0] + pieces[k][1]:
                    c.wait_recv()
            derive(close)

            def rest():
                for k in behind:
                    for c in pieces[k][0] + pieces[k][1]:
                        c.wait_recv()
                derive(distant)

            return rest

        def lifts(tables, slots):
            out = []
            for p in slots:
                table = tables[0 if p < 2 else 1 if p < 2 + px else 2]
                out.append((p, jnp.take_along_axis(table, AGX[p], axis=1, mode="promise_in_bounds")))
            return out

        def lift(e, found):
            for p, lifted in found:
                FIX[p] = CUR[e, 0, p] + lifted

        def receive(e):
            final = isinstance(e, int)
            share_done(e - 1, gs)
            landed = rings(e, 1) if final else halo(e)
            late_faces = [FACES.index((-1 if up else 1, 0))]
            late_corners = [k for k, d in enumerate(CORNERS) if d[0] == (-1 if up else 1)]
            slow = late_faces if final else late_faces + [len(FACES) + late_faces[0]] + [len(FACES) + 2 + k for k in late_corners]
            for k in range(len(landed)):
                if k not in slow:
                    landed[k].wait_recv()
            share_done(e - 1, gr)
            parts = [YB[e - 1, me_w]] + [GB[e - 1, k] for k in range(len(pairs))]
            while len(parts) > 1:
                parts = [sum(parts[k : k + 2][1:], parts[k]) for k in range(0, len(parts), 2)]
            total = parts[0]
            tables = [jnp.broadcast_to(total[k : k + 1], (2 * cy, tile)) for k in range(3)]
            if not final:
                unpack(e, [k for k in range(len(CORNERS)) if k not in late_corners])
            lift(e, lifts(tables, [p for p in range(px + 4) if p not in faraway]))
            ready = lifts(tables, faraway)

            def rest():
                for k in slow:
                    landed[k].wait_recv()
                if not final:
                    unpack(e, late_corners)
                lift(e, ready)

            return rest

        def begin_box(read, boxes, acc):
            for b, applied in operate(read, boxes, True):
                h = [COEF[first_rhs + c, b + 1] - applied[c] for c in range(phases)]
                for c in range(phases):
                    H[c, b] = h[c]
                out = product(b, scaled(b, h), ring_rows if b in inner else near_rows)
                for c in range(phases):
                    W1[c, b + 1] = out[c]
                if acc is not None and b in inner:
                    acc = gather(acc, b - 1, h[0])
            return acc

        def sweep(s, first):
            read = current(s)
            def improve(boxes):
                for b, applied in operate(lambda c, idx: W1[c, idx], boxes):
                    q = scaled(b, [H[c, b] - applied[c] for c in range(phases)])
                    out = product(b, q, near_rows if b in inner else None)
                    n = 2 * cy if b in inner else cy
                    for c in range(phases):
                        W2[c, b + 1, :n] = W1[c, b + 1, :n] + out[c]

            rest = opening(derive, close, distant) if first else receive(s)
            acc = begin_box(read, close, None if first else jnp.zeros((aggs, tile), F32))
            improve(order[:0])
            rest()
            acc = begin_box(read, distant, acc)
            if not first:
                for c in solve_coarse(s, acc):
                    c.start()
            improve(order[0:])
            done = []
            for b, applied in operate(lambda c, idx: W2[c, idx], order[1:-1]):
                done.append((b, product(b, scaled(b, [H[c, b] - applied[c] for c in range(phases)]), None)))
            for b, out in done:
                for c in range(phases):
                    CUR[s + 1, c, b + 1, :cy] = read(c, b + 1)[:cy] + (W2[c, b + 1, :cy] + out[c])
            first_face = [1, 0, 2, 3] if up else [0, 1, 2, 3]

            def send_all():
                ring = rings(s + 1, 3)
                for k in first_face:
                    ring[k].start()
                pack(s + 1)
                more = extras(s + 1)
                turn = [1, 4, 5, 0, 2, 3] if up else [0, 2, 3, 1, 4, 5]
                for k in turn:
                    more[k].start()

            def send_last():
                ring = rings(s + 1, 1)
                for k in first_face:
                    ring[k].start()

            if first:
                send_all()
            else:
                pl.when(s + 1 < SWEEPS)(send_all)
                pl.when(s + 1 == SWEEPS)(send_last)
            drain(s)
            if first:
                for c in coef + thin + aggregates:
                    c.wait_send()
                for c in aggregates:
                    c.wait_recv()

        def later(s, carry):
            sweep(s, False)
            return carry

        sweep(0, True)
        lax.fori_loop(1, SWEEPS, later, 0)
        rest = receive(SWEEPS)
        last = current(SWEEPS)
        for c in range(phases):
            for p in range(px):
                out_it[c, p] = last(c, p + 2)[:cy]

        def finish(boxes):
            for b, applied in operate(last, boxes):
                for c in range(phases):
                    out_res[c, b - 1] = COEF[first_rhs + c, b + 1, 0:cy] - applied[c][:cy]

        finish(close[1:])
        rest()
        finish(distant[:1])
        for c in rings(SWEEPS, 1):
            c.wait_send()

    for p in range(px + 4):
        FIX[p] = CUR[0, 0, p]

    @pl.when(odd == 1)
    def _():
        run(True)

    @pl.when(odd == 0)
    def _():
        run(False)


def hand_over(iterate, residual, out_it, out_res, sem):
    moves = [
        pltpu.make_async_copy(iterate, out_it, sem.at[0]),
        pltpu.make_async_copy(residual, out_res, sem.at[1]),
    ]
    for c in moves:
        c.start()
    for c in moves:
        c.wait()


def solution(mesh):
    nw, nn = mesh.shape["wide"], mesh.shape["narrow"]

    def per_device(rhs, start, trans, accum, coupling, well_cells, well_index, agg_map, tile_factors, coarse_inverse):
        phases, px, cy, tile = rhs.shape
        box = px + 2
        aggs = coarse_inverse.shape[0]
        conn = well_cells.size
        nch = 4 + phases * phases + phases
        vmem = pl.BlockSpec(memory_space=pltpu.VMEM)
        hbm = pl.BlockSpec(memory_space=pl.ANY)
        shape = jax.ShapeDtypeStruct(rhs.shape, F32)
        ring = (2 * cy, tile)
        dma = pltpu.SemaphoreType.DMA
        call = pl.pallas_call(
            functools.partial(body, nw, nn),
            out_shape=(pltpu.VMEM(rhs.shape, F32), pltpu.VMEM(rhs.shape, F32)),
            in_specs=[hbm] * 10,
            out_specs=(vmem, vmem),
            scratch_shapes=[
                pltpu.VMEM((nch, px + 4) + ring, F32),
                pltpu.VMEM((SWEEPS + 1, phases, px + 4) + ring, F32),
                pltpu.VMEM((px + 4,) + ring, F32),
                pltpu.VMEM((phases, px + 4) + ring, F32),
                pltpu.VMEM((phases, px + 4) + ring, F32),
                pltpu.VMEM((phases, box) + ring, F32),
                pltpu.VMEM((4 + 2 * phases, box) + ring, F32),
                pltpu.VMEM(tile_factors.shape, tile_factors.dtype),
                pltpu.VMEM((box, (cy // 2 + 2) * tile, 2 * tile), tile_factors.dtype),
                pltpu.VMEM(coarse_inverse.shape, F32),
                pltpu.VMEM((px * cy, tile), jnp.int32),
                pltpu.VMEM((px + 4,) + ring, jnp.int32),
                pltpu.VMEM(accum.shape, F32),
                pltpu.VMEM((1, conn), jnp.int32),
                pltpu.VMEM((1, conn), F32),
                pltpu.VMEM((SWEEPS, nw * nn - 1, 3, tile), F32),
                pltpu.VMEM((SWEEPS, nw, 3, tile), F32),
                pltpu.VMEM((cy, tile), F32),
                pltpu.VMEM((px, 1, tile), F32),
                pltpu.VMEM((SWEEPS, 2, 2, cy, tile), F32),
                pltpu.VMEM((SWEEPS, len(CORNERS), 2 * phases + 2, tile), F32),
                pltpu.VMEM((SWEEPS, len(CORNERS), 2 * phases + 2, tile), F32),
                dma((11,)),
                dma((SWEEPS + 1, len(DIRS) + 2)),
                dma((SWEEPS + 1, len(DIRS) + 2)),
                dma((14,)),
                dma((14,)),
                dma((SWEEPS,)),
                dma((SWEEPS,)),
                dma((len(DIRS),)),
                dma((len(DIRS),)),
                dma((2,)),
                dma((2,)),
                pltpu.SemaphoreType.REGULAR,
                pltpu.SemaphoreType.REGULAR((max(nw, nn),)),
            ],
            compiler_params=pltpu.CompilerParams(collective_id=0, has_side_effects=True),
            name="schwarz",
        )
        held = call(
            rhs, start, trans, accum,
            coupling.reshape((phases * phases,) + accum.shape),
            well_cells.reshape(1, -1), well_index.reshape(1, -1),
            agg_map.reshape(px * cy, tile), tile_factors, coarse_inverse)
        held = [pltpu.with_memory_space_constraint(x, pltpu.VMEM) for x in held]
        return pl.pallas_call(
            hand_over, out_shape=(shape, shape), in_specs=[vmem, vmem], out_specs=(hbm, hbm),
            scratch_shapes=[dma((2,))], name="hand_over",
        )(*held)

    return jax.shard_map(
        per_device,
        mesh=mesh,
        in_specs=(
            P(None, "wide", "narrow", None),
            P(None, "wide", "narrow", None),
            P(None, "wide", "narrow", None),
            P("wide", "narrow", None),
            P(None, None, "wide", "narrow", None),
            P("wide", "narrow", None),
            P("wide", "narrow", None),
            P("wide", "narrow", None),
            P("wide", "narrow", None, None),
            P(("wide", "narrow"), None),
        ),
        out_specs=(P(None, "wide", "narrow", None), P(None, "wide", "narrow", None)),
        check_vma=False,
    )
```
